16 devices in a mesh: dp: 2 (over y, z), sp: 8 (over x, core).
Axes of the slice: x: 4, y: 2, z: 1, core: 2. Of those that a mesh axis runs over, the one named last changes fastest.
The devices are a block of a 4x4x8 slice.
Arguments:
- x: bfloat16 [2048, 4096], P(('dp', 'sp')), parts along dimension 0
- gain: bfloat16 [4096], replicated
- wq: bfloat16 [4096, 4096], replicated
- wk: bfloat16 [4096, 512], replicated
- wv: bfloat16 [4096, 512], replicated
- wo: bfloat16 [4096, 4096], replicated
Outputs:
- output: bfloat16 [2048, 4096], P(('dp', 'sp')), parts along dimension 0
There are 2 independent parts. The reference program is written for one: setup_inputs(seed, part) draws one part's arguments, and reference() takes and returns one part's arrays. A program takes and returns all parts, laid end to end along the dimension named above; an argument that names none is the same for every part.
All inputs are finite; a program needn't handle non-finite values.
Results may differ from the reference program's by a relative error of at most 0.012.
Values are sent between devices in bfloat16 or wider.
A program may use at most 768 MiB of HBM per device.

```python
import jax
import jax.numpy as jnp
from jax import lax

ROWS = 1024
D = 4096
HEADS = 32
KV_HEADS = 4
HEAD = 128
THETA = 10000


def setup_inputs(seed: int = 0, part: int = 0) -> dict:
    kx, kn, kq, kk, kv, ko = jax.random.split(jax.random.key(seed), 6)

    def weights(key, rows, columns):
        return jax.random.normal(key, (rows, columns), jnp.float32) * rows**-0.5

    drawn = {
        "x": jax.random.normal(jax.random.fold_in(kx, part), (ROWS, D), jnp.float32),
        "gain": 1 + 0.1 * jax.random.normal(kn, (D,), jnp.float32),
        "wq": 2 * weights(kq, D, HEADS * HEAD),
        "wk": 2 * weights(kk, D, KV_HEADS * HEAD),
        "wv": 4 * weights(kv, D, KV_HEADS * HEAD),
        "wo": weights(ko, HEADS * HEAD, D),
    }
    return {k: v.astype(jnp.bfloat16) for k, v in drawn.items()}


def normed(x, gain):
    wide = x.astype(jnp.float32)
    scale = lax.rsqrt(jnp.mean(wide * wide, -1, keepdims=True) + 1e-6)
    return (wide * scale * gain.astype(jnp.float32)).astype(jnp.bfloat16)


def turned(t, place, theta):
    half = t.shape[-1] // 2
    angle = place.astype(jnp.float32)[:, None] * theta ** (-jnp.arange(half, dtype=jnp.float32) / half)
    cos, sin = jnp.cos(angle)[:, None], jnp.sin(angle)[:, None]
    a, b = t[..., :half].astype(jnp.float32), t[..., half:].astype(jnp.float32)
    return jnp.concatenate([a * cos - b * sin, b * cos + a * sin], -1).astype(jnp.bfloat16)


def matmul(a, w):
    return jnp.dot(a, w, preferred_element_type=jnp.float32).astype(jnp.bfloat16)


def einsum(form, a, b):
    return jnp.einsum(form, a.astype(jnp.float32), b.astype(jnp.float32))


def attention(q, k, v):
    scores = einsum("tgsd,ugd->gstu", q, k) * q.shape[-1] ** -0.5
    token = jnp.arange(q.shape[0])
    scores = jnp.where(token[:, None] >= token, scores, -jnp.inf)
    weights = jax.nn.softmax(scores, -1).astype(jnp.bfloat16)
    return einsum("gstu,ugd->tgsd", weights, v).astype(jnp.bfloat16)


def reference(x, gain, wq, wk, wv, wo):
    a, place = normed(x, gain), jnp.arange(ROWS)
    q = turned(matmul(a, wq).reshape(ROWS, HEADS, HEAD), place, THETA).reshape(ROWS, KV_HEADS, -1, HEAD)
    k = turned(matmul(a, wk).reshape(ROWS, KV_HEADS, HEAD), place, THETA)
    v = matmul(a, wv).reshape(ROWS, KV_HEADS, HEAD)
    seen = attention(q, k, v).reshape(ROWS, HEADS * HEAD)
    return (x.astype(jnp.float32) + jnp.dot(seen, wo, preferred_element_type=jnp.float32)).astype(jnp.bfloat16)
```

```python
import functools

import jax
import jax.numpy as jnp
from jax import lax
from jax.experimental import pallas as pl
from jax.experimental.pallas import tpu as pltpu
from jax.sharding import PartitionSpec as P

HEAD = 128
THETA = 10000
LOG2E = 1.4426950408889634
LOG2T = 13.287712379549449
HIDDEN = -2e30
MESH = pl.DeviceIdType.MESH
F32, BF16 = jnp.float32, jnp.bfloat16


def _dot(a, b, ca, cb):
    return lax.dot_general(a, b, (((ca,), (cb,)), ((), ())), preferred_element_type=F32)


def _kernel(n, x_hbm, gain_ref, wq_hbm, wk_hbm, wv_hbm, wo_hbm, out_hbm,
            xb, a, xr, wkv, wqb, wob, q, kv, seen, ys, top_s, mix_s, cos_s, sin_s,
            x_sem, wkv_sem, wq_sem, wo_sem, a_send, a_recv, r_sem, r_send, r_recv,
            k_send, k_wrap, k_relay, k_recv, s_send, s_recv, y_sem, y_send, y_recv):
    own, d = x_hbm.shape
    toks = 2 * own
    half = wqb.shape[0] * wqb.shape[2]
    part = wqb.shape[2]
    nq = wqb.shape[0]
    hk = kv.shape[1]
    kc = hk * HEAD
    group = q.shape[1] // toks
    me = lax.axis_index("sp")
    chip, core = lax.div(me, 2), lax.rem(me, 2)
    mate = {"sp": chip * 2 + 1 - core}

    def peer(at):
        return {"sp": at * 2 + core}

    mine = pl.multiple_of(core * own, own)
    theirs = pl.multiple_of((1 - core) * own, own)
    cols = pl.multiple_of(core * half, half)
    mate_cols = pl.multiple_of((1 - core) * half, half)

    barrier = pltpu.get_barrier_semaphore()
    pl.semaphore_signal(barrier, inc=1, device_id=mate, device_id_type=MESH)
    for i in range(1, n):
        pl.semaphore_signal(barrier, inc=1, device_id=peer(lax.rem(chip + i, n)), device_id_type=MESH)

    rows = own // x_sem.shape[0]

    def x_copy(i):
        return pltpu.make_async_copy(x_hbm.at[pl.ds(i * rows, rows)], xb.at[pl.ds(i * rows, rows)], x_sem.at[i])

    k_copy = pltpu.make_async_copy(wk_hbm.at[:, pl.ds(pl.multiple_of(core * kc, kc), kc)], wkv.at[:, pl.ds(0, kc)], wkv_sem.at[0])
    v_copy = pltpu.make_async_copy(wv_hbm.at[:, pl.ds(pl.multiple_of(core * kc, kc), kc)], wkv.at[:, pl.ds(kc, kc)], wkv_sem.at[1])

    def q_copy(i):
        return pltpu.make_async_copy(wq_hbm.at[:, pl.ds(pl.multiple_of(cols + i * part, part), part)], wqb.at[i], wq_sem.at[i])

    def o_copy(i):
        return pltpu.make_async_copy(wo_hbm.at[:, pl.ds(pl.multiple_of(cols + i * part, part), part)], wob.at[i], wo_sem.at[i])

    r_copy = pltpu.make_async_copy(x_hbm.at[:, pl.ds(cols, half)], xr.at[pl.ds(mine, own)], r_sem)
    for i in range(x_sem.shape[0]):
        x_copy(i).start()
    k_copy.start()
    v_copy.start()
    for i in range(nq):
        q_copy(i).start()
    r_copy.start()
    for i in range(nq):
        o_copy(i).start()

    lane = lax.broadcasted_iota(jnp.int32, (toks, HEAD), 1)
    place = lax.broadcasted_iota(jnp.int32, (toks, HEAD), 0) + chip * toks
    turn = lax.rem(lane, HEAD // 2).astype(F32) * (-LOG2T / (HEAD // 2))
    angle = place.astype(F32) * jnp.exp2(turn)
    cos_s[...] = jnp.cos(angle)
    sin_s[...] = jnp.where(lane < HEAD // 2, -1.0, 1.0) * jnp.sin(angle)

    def turned(t, cos, sin):
        t = t.astype(BF16).astype(F32)
        return (t * cos + pltpu.roll(t, HEAD // 2, 1) * sin).astype(BF16)

    def a_copy(i, at):
        here = pl.ds(pl.multiple_of(at + i * rows, rows), rows)
        return pltpu.make_async_remote_copy(a.at[here], a.at[here], a_send.at[i], a_recv.at[i], device_id=mate, device_id_type=MESH)

    gain = gain_ref[...].astype(F32)
    pl.semaphore_wait(barrier, n)
    for i in range(x_sem.shape[0]):
        x_copy(i).wait()
        wide = xb[pl.ds(i * rows, rows), :].astype(F32)
        scale = lax.rsqrt(jnp.mean(wide * wide, -1, keepdims=True) + 1e-6)
        a[pl.ds(pl.multiple_of(mine + i * rows, rows), rows), :] = (wide * scale * gain).astype(BF16)
        a_copy(i, mine).start()
    r_give = pltpu.make_async_remote_copy(x_hbm.at[:, pl.ds(mate_cols, half)], xr.at[pl.ds(mine, own)], r_send, r_recv, device_id=mate,
                                          device_id_type=MESH)
    r_give.start()

    def piece(sem_s, sem_r, block, t, h, to):
        ref = kv.at[block, h, t]
        return pltpu.make_async_remote_copy(ref, ref, sem_s, sem_r, device_id=peer(to), device_id_type=MESH)

    def own_next(t, h):
        return piece(k_send.at[t, h], k_recv.at[chip, t, h], chip, t, h, lax.rem(chip + 1, n))

    def own_wrap(t, h):
        return piece(k_wrap.at[t, h], k_recv.at[chip, t, h], chip, t, h, n - 1)

    def relay(t, h):
        before = lax.rem(chip + n - 1, n)
        return piece(k_relay.at[t, h], k_recv.at[before, t, h], before, t, h, lax.rem(chip + 1, n))

    def arrived(block, t, h):
        piece(k_send.at[t, h], k_recv.at[block, t, h], block, t, h, chip).wait_recv()

    sends, wraps, relays = chip < n - 1, chip == 0, (chip > 0) & (chip < n - 1)

    def keys_values(t):
        here = pl.ds(pl.multiple_of(t * own, own), own)
        r = _dot(a[here, :], wkv[...], 1, 0)
        cos, sin = cos_s[here, :], sin_s[here, :]
        for h in range(hk):
            kv[chip, h, t, 0] = turned(r[:, h * HEAD : (h + 1) * HEAD], cos, sin)
            kv[chip, h, t, 1] = r[:, kc + h * HEAD : kc + (h + 1) * HEAD].astype(BF16).T

        @pl.when(sends)
        def _():
            for h in range(hk):
                own_next(t, h).start()

        @pl.when(wraps)
        def _():
            for h in range(hk):
                own_wrap(t, h).start()

    k_copy.wait()
    v_copy.wait()

    def half_step(i, _):
        @pl.when(i == 1)
        def _():
            for j in range(x_sem.shape[0]):
                a_copy(j, theirs).wait_recv()

        keys_values(lax.rem(core + i, 2))

    lax.fori_loop(0, 2, half_step, None)

    def queries(i, _):
        q_copy(i).wait()
        r = _dot(a[...], wqb[i], 1, 0)
        heads = part // HEAD
        cos, sin = cos_s[...], sin_s[...]
        for j in range(heads):
            at = i * heads + j
            q[lax.div(at, group), pl.ds(pl.multiple_of(lax.rem(at, group) * toks, toks), toks), :] = turned(
                r[:, j * HEAD : (j + 1) * HEAD], cos, sin)

        @pl.when(relays)
        def _():
            t, h = lax.rem(core + lax.div(i, hk), 2), lax.rem(i, hk)
            arrived(chip - 1, t, h)
            relay(t, h).start()

    lax.fori_loop(0, nq, queries, None)

    e = HEAD**-0.5 * LOG2E
    wide = 2 * toks
    strips = q.shape[1] // wide
    ones = jnp.ones((8, toks), BF16)

    def s_copy(h, s, at):
        here = pl.ds(pl.multiple_of(at + (h * group + s * 2) * HEAD, 2 * HEAD), 2 * HEAD)
        ref = seen.at[:, here]
        return pltpu.make_async_remote_copy(ref, ref, s_send.at[h, s], s_recv.at[h, s], device_id=mate, device_id_type=MESH)

    def block(h, j, first):
        keys = jnp.concatenate([kv[j, h, 0, 0], kv[j, h, 1, 0]], axis=0)
        values = jnp.concatenate([jnp.concatenate([kv[j, h, 0, 1], kv[j, h, 1, 1]], axis=1), ones], axis=0)
        scores = [_dot(keys, q[h, pl.ds(s * wide, wide), :], 1, 1) for s in range(strips)]
        if first:
            ok = lax.rem(lax.broadcasted_iota(jnp.int32, (toks, wide), 1), toks) >= lax.broadcasted_iota(jnp.int32, (toks, wide), 0)
        weights, keeps = [], []
        for s, sc in enumerate(scores):
            at = pl.ds(s * wide, wide)
            if first:
                sc = jnp.where(ok, sc, HIDDEN)
                top = sc.max(axis=0, keepdims=True)
            else:
                old = top_s[:, at]
                top = jnp.maximum(old, sc.max(axis=0, keepdims=True))
                keeps.append(jnp.exp2((old - top) * e))
            top_s[:, at] = top
            weights.append(jnp.exp2((sc - top) * e).astype(BF16))
        for s, p in enumerate(weights):
            at = pl.ds(s * wide, wide)
            new = _dot(values, p, 1, 0)
            mix_s[:, at] = new if first else mix_s[:, at] * keeps[s] + new

    def head(h, _):
        block(h, chip, True)

        def before(i, _):
            j = jnp.where(i == 0, chip - 1, i - 1)

            @pl.when(jnp.logical_not(relays & (i == 0)))
            def _():
                for t in range(2):
                    arrived(j, t, h)

            block(h, j, False)

        lax.fori_loop(0, chip, before, None)
        for s in range(strips):
            at = pl.ds(s * wide, wide)
            o = (mix_s[:HEAD, at] * (1 / mix_s[HEAD : HEAD + 1, at])).astype(BF16).T
            for j in range(2):
                seen[:, pl.ds(pl.multiple_of(cols + (h * group + s * 2 + j) * HEAD, HEAD), HEAD)] = o[j * toks : (j + 1) * toks]
            s_copy(h, s, cols).start()

    lax.fori_loop(0, hk, head, None)

    r_copy.wait()
    r_give.wait_recv()
    for h in range(hk):
        for s in range(strips):
            s_copy(h, s, mate_cols).wait_recv()

    def y_own(i):
        at = pl.multiple_of(i * part, part)
        return pltpu.make_async_copy(ys.at[pl.ds(mine, own), pl.ds(at, part)], out_hbm.at[:, pl.ds(pl.multiple_of(cols + at, part), part)],
                                     y_sem.at[i])

    def y_give(i, side):
        at = pl.multiple_of(i * part, part)
        return pltpu.make_async_remote_copy(ys.at[pl.ds(theirs, own), pl.ds(at, part)],
                                            out_hbm.at[:, pl.ds(pl.multiple_of(side + at, part), part)],
                                            y_send.at[i], y_recv.at[i], device_id=mate, device_id_type=MESH)

    def output(i, _):
        o_copy(i).wait()
        at = pl.ds(pl.multiple_of(i * part, part), part)
        r = _dot(seen[...], wob[i], 1, 0)
        ys[:, at] = (xr[:, at].astype(F32) + r).astype(BF16)
        y_give(i, cols).start()
        y_own(i).start()

    lax.fori_loop(0, nq, output, None)

    for i in range(nq):
        y_own(i).wait()
        y_give(i, cols).wait_send()
        y_give(i, mate_cols).wait_recv()
    for i in range(x_sem.shape[0]):
        a_copy(i, mine).wait_send()
    r_give.wait_send()
    for h in range(hk):
        for s in range(strips):
            s_copy(h, s, cols).wait_send()

    def finish(flag, copy):
        @pl.when(flag)
        def _():
            for t in range(2):
                for h in range(hk):
                    copy(t, h).wait_send()

    finish(sends, own_next)
    finish(wraps, own_wrap)
    finish(relays, relay)


def _call(x, gain, wq, wk, wv, wo, devices):
    own, d = x.shape
    n, toks = devices // 2, 2 * own
    half, kc = wq.shape[1] // 2, wk.shape[1] // 2
    nq = 4
    part = half // nq
    hk = kc // HEAD
    group = half // kc
    cols = group * toks
    strips = cols // (2 * toks)
    dma = pltpu.SemaphoreType.DMA
    any_ = pl.BlockSpec(memory_space=pltpu.HBM)
    return pl.pallas_call(
        functools.partial(_kernel, n),
        out_shape=jax.ShapeDtypeStruct((own, d), BF16),
        in_specs=[any_, pl.BlockSpec(memory_space=pltpu.VMEM), any_, any_, any_, any_],
        out_specs=any_,
        scratch_shapes=[
            pltpu.VMEM((own, d), BF16),
            pltpu.VMEM((toks, d), BF16),
            pltpu.VMEM((toks, half), BF16),
            pltpu.VMEM((d, 2 * kc), BF16),
            pltpu.VMEM((nq, d, part), BF16),
            pltpu.VMEM((nq, d, part), BF16),
            pltpu.VMEM((hk, cols, HEAD), BF16),
            pltpu.VMEM((n, hk, 2, 2, HEAD, HEAD), BF16),
            pltpu.VMEM((toks, d), BF16),
            pltpu.VMEM((toks, half), BF16),
            pltpu.VMEM((1, cols), F32),
            pltpu.VMEM((HEAD + 8, cols), F32),
            pltpu.VMEM((toks, HEAD), F32),
            pltpu.VMEM((toks, HEAD), F32),
            dma((4,)), dma((2,)), dma((nq,)), dma((nq,)),
            dma((4,)), dma((4,)), dma, dma, dma,
            dma((2, hk)), dma((2, hk)), dma((2, hk)), dma((n, 2, hk)),
            dma((hk, strips)), dma((hk, strips)),
            dma((nq,)), dma((nq,)), dma((nq,)),
        ],
        compiler_params=pltpu.CompilerParams(collective_id=0, has_side_effects=True, vmem_limit_bytes=60 * 2**20),
    )(x, gain, wq, wk, wv, wo)


def solution(mesh):
    devices = mesh.shape["sp"]

    def step(x, gain, wq, wk, wv, wo):
        return _call(x, gain[None], wq, wk, wv, wo, devices)

    tokens, whole = P(("dp", "sp"), None), P(None, None)
    return jax.shard_map(
        step,
        mesh=mesh,
        in_specs=(tokens, P(None), whole, whole, whole, whole),
        out_specs=tokens,
        check_vma=False,
    )
```

```python
import functools

import jax
import jax.numpy as jnp
from jax import lax
from jax.experimental import pallas as pl
from jax.experimental.pallas import tpu as pltpu
from jax.sharding import PartitionSpec as P

HEAD = 128
THETA = 10000
LOG2E = 1.4426950408889634
LOG2T = 13.287712379549449
HIDDEN = -2e30
VMEM = 60 * 2**20
MESH = pl.DeviceIdType.MESH
F32, BF16 = jnp.float32, jnp.bfloat16
scope = jax.named_scope


def _dot(a, b, ca=1, cb=0):
    return lax.dot_general(a, b, (((ca,), (cb,)), ((), ())), preferred_element_type=F32)


def _kernel(n, x_hbm, gain_hbm, wq_hbm, wk_hbm, wv_hbm, wo_hbm, out_ref,
            gain_s, xb, a, xr, wkv, wqb, wob, raw, q, kv, seen, acc, ys, top_s, mix_s, cos_s, sin_s,
            g_sem, x_sem, wkv_sem, wq_sem, wo_sem, a_send, a_recv, r_sem, r_send, r_recv,
            k_next, k_wrap, k_back, k_relay, k_edge, k_recv, s_send, s_recv, y_send, y_recv):
    own, d = x_hbm.shape
    toks = 2 * own
    nq, _, part = wqb.shape
    half = nq * part
    hk = kv.shape[1]
    kc = hk * HEAD
    group = q.shape[1] // toks
    me = lax.axis_index("sp")
    chip, core = lax.div(me, 2), lax.rem(me, 2)
    mate = {"sp": chip * 2 + 1 - core}

    def peer(at):
        return {"sp": at * 2 + core}

    mine = pl.multiple_of(core * own, own)
    theirs = pl.multiple_of((1 - core) * own, own)
    cols = pl.multiple_of(core * half, half)
    mate_cols = pl.multiple_of((1 - core) * half, half)

    barrier = pltpu.get_barrier_semaphore()
    pl.semaphore_signal(barrier, inc=1, device_id=mate, device_id_type=MESH)
    for i in range(1, n):
        pl.semaphore_signal(barrier, inc=1, device_id=peer(lax.rem(chip + i, n)), device_id_type=MESH)

    nx = x_sem.shape[0]
    rows = own // nx
    kcols = pl.ds(pl.multiple_of(core * kc, kc), kc)

    def x_copy(i):
        return pltpu.make_async_copy(x_hbm.at[pl.ds(i * rows, rows)], xb.at[pl.ds(i * rows, rows)], x_sem.at[i])

    def q_copy(i):
        return pltpu.make_async_copy(wq_hbm.at[:, pl.ds(pl.multiple_of(cols + i * part, part), part)], wqb.at[i], wq_sem.at[i])

    def o_copy(i):
        return pltpu.make_async_copy(wo_hbm.at[:, pl.ds(pl.multiple_of(cols + i * part, part), part)], wob.at[i], wo_sem.at[i])

    g_copy = pltpu.make_async_copy(gain_hbm, gain_s, g_sem)
    k_copy = pltpu.make_async_copy(wk_hbm.at[:, kcols], wkv.at[:, pl.ds(0, kc)], wkv_sem.at[0])
    v_copy = pltpu.make_async_copy(wv_hbm.at[:, kcols], wkv.at[:, pl.ds(kc, kc)], wkv_sem.at[1])
    r_copy = pltpu.make_async_copy(x_hbm.at[:, pl.ds(cols, half)], xr.at[pl.ds(mine, own)], r_sem)
    r_give = pltpu.make_async_remote_copy(x_hbm.at[:, pl.ds(mate_cols, half)], xr.at[pl.ds(mine, own)], r_send, r_recv, device_id=mate,
                                          device_id_type=MESH)
    g_copy.start()
    for i in range(nx):
        x_copy(i).start()
    k_copy.start()

    lane = lax.broadcasted_iota(jnp.int32, (toks, HEAD), 1)
    place = lax.broadcasted_iota(jnp.int32, (toks, HEAD), 0) + chip * toks
    turn = lax.rem(lane, HEAD // 2).astype(F32) * (-LOG2T / (HEAD // 2))
    angle = place.astype(F32) * jnp.exp2(turn)
    cos_s[...] = jnp.cos(angle)
    sin_s[...] = jnp.where(lane < HEAD // 2, -1.0, 1.0) * jnp.sin(angle)
    v_copy.start()

    def turned(t, cos, sin):
        t = t.astype(BF16).astype(F32)
        return (t * cos + pltpu.roll(t, HEAD // 2, 1) * sin).astype(BF16)

    def a_copy(i, at):
        here = pl.ds(pl.multiple_of(at + i * rows, rows), rows)
        return pltpu.make_async_remote_copy(a.at[here], a.at[here], a_send.at[i], a_recv.at[i], device_id=mate, device_id_type=MESH)

    with scope("barrier"):
        g_copy.wait()
        pl.semaphore_wait(barrier, n)
    gain = gain_s[...].astype(F32)[None]
    for i in range(nx):
        with scope("x_wait"):
            x_copy(i).wait()
        if i == 0:
            q_copy(0).start(priority=1)
        wide = xb[pl.ds(i * rows, rows), :].astype(F32)
        scale = lax.rsqrt(jnp.mean(wide * wide, -1, keepdims=True) + 1e-6)
        a[pl.ds(pl.multiple_of(mine + i * rows, rows), rows), :] = (wide * scale * gain).astype(BF16)
        a_copy(i, mine).start()

    def piece(sem, block, t, h, to):
        ref = kv.at[block, h, t]
        return pltpu.make_async_remote_copy(ref, ref, sem, k_recv.at[block, t, h], device_id=peer(to), device_id_type=MESH)

    last = n - 1
    sends, wraps, backs = chip < last, chip == 0, chip == 1
    relays, edges = (chip > 0) & (chip < last), (chip == 0) | (chip == last)
    edge_block, edge_to = jnp.where(chip == 0, 1, 0), jnp.where(chip == 0, last, last - 1)
    prev, nxt = lax.rem(chip + n - 1, n), lax.rem(chip + 1, n)

    def to_next(t, h):
        return piece(k_next.at[t, h], chip, t, h, nxt)

    def to_last(t, h):
        return piece(k_wrap.at[t, h], chip, t, h, last)

    def to_first(t):
        return piece(k_back.at[t], chip, t, 1, 0)

    def relay(t):
        return piece(k_relay.at[t], prev, t, 0, nxt)

    def edge(t):
        return piece(k_edge.at[t], edge_block, t, 1, edge_to)

    def arrived(block, t, h):
        piece(k_edge.at[t], block, t, h, chip).wait_recv()

    def when(flag, *copies):
        @pl.when(flag)
        def _():
            for copy in copies:
                copy.start()

    def keys_values(t):
        here = pl.ds(pl.multiple_of(t * own, own), own)
        r = _dot(a[here, :], wkv[...])
        cos, sin = cos_s[here, :], sin_s[here, :]
        for h in range(hk):
            kv[chip, h, t, 0] = turned(r[:, h * HEAD : (h + 1) * HEAD], cos, sin)
            kv[chip, h, t, 1] = r[:, kc + h * HEAD : kc + (h + 1) * HEAD].astype(BF16).T

    t0, t1 = core, 1 - core
    with scope("kv_wait"):
        k_copy.wait()
        v_copy.wait()
    q_copy(1).start(priority=1)

    def half_step(i, _):
        @pl.when(i == 1)
        def _():
            with scope("a_wait"):
                for j in range(nx):
                    a_copy(j, theirs).wait_recv()

        t = lax.rem(core + i, 2)
        with scope("kv_mm"):
            keys_values(t)
        when(sends, to_next(t, 0))
        when(wraps, to_last(t, 1), to_last(t, 0))
        when(backs, to_first(t))

    lax.fori_loop(0, 2, half_step, None)
    when(sends, to_next(t0, 1))
    q_copy(2).start(priority=1)
    q_copy(3).start(priority=1)

    heads = part // HEAD

    def turn_queries(i):
        for j in range(heads):
            at = i * heads + j
            q[at // group, pl.ds((at % group) * toks, toks), :] = turned(raw[i % 2, :, j * HEAD : (j + 1) * HEAD], cos_s[...], sin_s[...])

    def relay_step(t):
        @pl.when(relays)
        def _():
            with scope("relay_wait"):
                arrived(prev, t, 0)
            relay(t).start()

        @pl.when(edges)
        def _():
            with scope("edge_wait"):
                arrived(edge_block, t, 1)
            edge(t).start()

    for i in range(nq):
        with scope("q_wait"):
            q_copy(i).wait()
        o_copy(i).start(priority=1)
        with scope("q_mm"):
            raw[i % 2] = _dot(a[...], wqb[i]).astype(BF16)
            if i:
                turn_queries(i - 1)
        if i == 0:
            r_copy.start(priority=1)
            r_give.start()
        if i == 1:
            relay_step(t0)
        if i == 2:
            relay_step(t1)
            when(sends, to_next(t1, 1))
    turn_queries(nq - 1)

    e = HEAD**-0.5 * LOG2E
    wide = 2 * toks
    strips = q.shape[1] // wide

    def attend(h, blocks, first):
        keys = jnp.concatenate([kv[j, h, t, 0] for j in blocks for t in range(2)], axis=0)
        values = jnp.concatenate([kv[j, h, t, 1] for j in blocks for t in range(2)], axis=1)
        values = jnp.concatenate([values, jnp.ones((8, values.shape[1]), BF16)], axis=0)

        def score(s):
            return _dot(keys, q[h, pl.ds(s * wide, wide), :], 1, 1)

        if first:
            ok = lax.rem(lax.broadcasted_iota(jnp.int32, (toks, wide), 1), toks) >= lax.broadcasted_iota(jnp.int32, (toks, wide), 0)
        ahead = score(0)
        for s in range(strips):
            at = pl.ds(s * wide, wide)
            sc = ahead
            if s + 1 < strips:
                ahead = score(s + 1)
            if first:
                here = jnp.where(ok, sc[:toks], HIDDEN)
                sc = here if len(blocks) == 1 else jnp.concatenate([here, sc[toks:]], axis=0)
            top = sc.max(axis=0, keepdims=True)
            if not first:
                old = top_s[h, :, at]
                top = jnp.maximum(old, top)
                keep = jnp.exp2((old - top) * e)
            top_s[h, :, at] = top
            new = _dot(values, jnp.exp2((sc - top) * e).astype(BF16))
            mix_s[h, :, at] = new if first else mix_s[h, :, at] * keep + new

    def near(h, _):
        @pl.when(chip == 0)
        def _():
            with scope("att_1f"):
                attend(h, [chip], True)

        @pl.when(chip > 0)
        def _():
            @pl.when(jnp.logical_not(relays & (h == 0)))
            def _():
                with scope("arrive"):
                    for t in range(2):
                        arrived(prev, t, h)

            with scope("att_2f"):
                attend(h, [chip, prev], True)

    def s_copy(h, s):
        ref = (h, slice(None), pl.ds(s * 2 * HEAD, 2 * HEAD))
        return pltpu.make_async_remote_copy(seen.at[(0, *ref)], seen.at[(1, *ref)], s_send.at[h, s], s_recv.at[h, s], device_id=mate,
                                            device_id_type=MESH)

    def far(h, _):
        @pl.when(chip == 2)
        def _():
            with scope("arrive"):
                for t in range(2):
                    arrived(0, t, h)
            with scope("att_1"):
                attend(h, [0], False)

        @pl.when(chip == 3)
        def _():
            @pl.when(h == 0)
            def _():
                for t in range(2):
                    arrived(0, t, h)

            with scope("arrive"):
                for t in range(2):
                    arrived(1, t, h)
            with scope("att_2"):
                attend(h, [0, 1], False)

        with scope("finish"):
            eye = (lax.broadcasted_iota(jnp.int32, (toks, toks), 0) == lax.broadcasted_iota(jnp.int32, (toks, toks), 1)).astype(BF16)
            for s in range(strips):
                at = pl.ds(s * wide, wide)
                o = (mix_s[h, :HEAD, at] * (1 / mix_s[h, HEAD : HEAD + 1, at])).astype(BF16)
                two = jnp.concatenate([o[:, :toks], o[:, toks:]], axis=0)
                seen[0, h, :, pl.ds(s * 2 * HEAD, 2 * HEAD)] = _dot(eye, two, 1, 1).astype(BF16)
            for s in range(strips):
                s_copy(h, s).start()

    lax.fori_loop(0, hk, near, None)
    lax.fori_loop(0, hk, far, None)

    def weight(i, side, h):
        return wob[i, pl.ds(pl.multiple_of(side + h * group * HEAD, group * HEAD), group * HEAD), :]

    def y_give(i, rows_at, side):
        return pltpu.make_async_remote_copy(ys.at[rows_at, pl.ds(i * part, part)],
                                            out_ref.at[:, pl.ds(pl.multiple_of(side + i * part, part), part)],
                                            y_send.at[i], y_recv.at[i], device_id=mate, device_id_type=MESH)

    def early(i, rows_at):
        r = _dot(seen[0, 0, rows_at, :], weight(i, cols, 0)) + _dot(seen[0, 1, rows_at, :], weight(i, cols, 1))
        return r + _dot(seen[1, 0, rows_at, :], weight(i, mate_cols, 0))

    def late(i, rows_at):
        return _dot(seen[1, 1, rows_at, :], weight(i, mate_cols, 1))

    with scope("r_wait"):
        r_copy.wait()
        r_give.wait_recv()
        for s in range(strips):
            s_copy(0, s).wait_recv()
    every = pl.ds(0, toks)
    begun = acc.shape[1] // part
    for i in range(begun):
        with scope("o_wait"):
            o_copy(i).wait()
        with scope("o_early"):
            acc[:, i * part : (i + 1) * part] = xr[:, i * part : (i + 1) * part].astype(F32) + early(i, every)
    with scope("seen_wait"):
        for s in range(strips):
            s_copy(1, s).wait_recv()
    for i in range(nq):
        at = pl.ds(i * part, part)
        to = pl.ds(pl.multiple_of(cols + i * part, part), part)
        if i >= begun:
            with scope("o_wait"):
                o_copy(i).wait()
        if i + 1 < nq:
            with scope("o_mm"):
                if i < begun:
                    y = acc[:, at] + late(i, every)
                else:
                    y = xr[:, at].astype(F32) + early(i, every) + late(i, every)
                ys[:, at] = y.astype(BF16)
            y_give(i, pl.ds(theirs, own), cols).start()
            out_ref[:, to] = ys[pl.ds(mine, own), at]
        else:
            with scope("o_theirs"):
                it = pl.ds(theirs, own)
                ys[it, at] = (xr[it, at].astype(F32) + early(i, it) + late(i, it)).astype(BF16)
            y_give(i, it, cols).start()
            with scope("o_mine"):
                it = pl.ds(mine, own)
                out_ref[:, to] = (xr[it, at].astype(F32) + early(i, it) + late(i, it)).astype(BF16)

    with scope("y_wait"):
        for i in range(nq):
            y_give(i, pl.ds(theirs, own), cols).wait_send()
            y_give(i, pl.ds(theirs, own), mate_cols).wait_recv()
    for i in range(nx):
        a_copy(i, mine).wait_send()
    r_give.wait_send()
    for h in range(hk):
        for s in range(strips):
            s_copy(h, s).wait_send()

    def finish(flag, *copies):
        @pl.when(flag)
        def _():
            for copy in copies:
                copy.wait_send()

    both = [(t, h) for t in range(2) for h in range(hk)]
    finish(sends, *(to_next(t, h) for t, h in both))
    finish(wraps, *(to_last(t, h) for t, h in both))
    finish(backs, *(to_first(t) for t in range(2)))
    finish(relays, *(relay(t) for t in range(2)))
    finish(edges, *(edge(t) for t in range(2)))


def _call(x, gain, wq, wk, wv, wo, devices):
    own, d = x.shape
    n, toks = devices // 2, 2 * own
    half, kc = wq.shape[1] // 2, wk.shape[1] // 2
    nq, nx = 4, 4
    part = half // nq
    hk, group = kc // HEAD, half // kc
    cols = group * toks
    strips = group // 2
    if (n, hk) != (4, 2):
        raise ValueError("group size")
    dma = pltpu.SemaphoreType.DMA
    any_ = pl.BlockSpec(memory_space=pltpu.HBM)
    return pl.pallas_call(
        functools.partial(_kernel, n),
        out_shape=pltpu.VMEM((own, d), BF16),
        in_specs=[any_] * 6,
        out_specs=pl.BlockSpec(memory_space=pltpu.VMEM),
        scratch_shapes=[
            pltpu.VMEM((d,), BF16),
            pltpu.VMEM((own, d), BF16),
            pltpu.VMEM((toks, d), BF16),
            pltpu.VMEM((toks, half), BF16),
            pltpu.VMEM((d, 2 * kc), BF16),
            pltpu.VMEM((nq, d, part), BF16),
            pltpu.VMEM((nq, d, part), BF16),
            pltpu.VMEM((2, toks, part), BF16),
            pltpu.VMEM((hk, cols, HEAD), BF16),
            pltpu.VMEM((n, hk, 2, 2, HEAD, HEAD), BF16),
            pltpu.VMEM((2, hk, toks, group * HEAD), BF16),
            pltpu.VMEM((toks, 2 * part), F32),
            pltpu.VMEM((toks, half), BF16),
            pltpu.VMEM((hk, 1, cols), F32),
            pltpu.VMEM((hk, HEAD + 8, cols), F32),
            pltpu.VMEM((toks, HEAD), F32),
            pltpu.VMEM((toks, HEAD), F32),
            dma, dma((nx,)), dma((2,)), dma((nq,)), dma((nq,)),
            dma((nx,)), dma((nx,)), dma, dma, dma,
            dma((2, hk)), dma((2, hk)), dma((2,)), dma((2,)), dma((2,)), dma((n, 2, hk)),
            dma((hk, strips)), dma((hk, strips)),
            dma((nq,)), dma((nq,)),
        ],
        compiler_params=pltpu.CompilerParams(collective_id=0, has_side_effects=True, vmem_limit_bytes=VMEM),
    )(x, gain, wq, wk, wv, wo)


def solution(mesh):
    devices = mesh.shape["sp"]

    def step(x, gain, wq, wk, wv, wo):
        return _call(x, gain, wq, wk, wv, wo, devices)

    tokens, whole = P(("dp", "sp"), None), P(None, None)
    return jax.shard_map(
        step,
        mesh=mesh,
        in_specs=(tokens, P(None), whole, whole, whole, whole),
        out_specs=tokens,
        check_vma=False,
    )
```

```python
import functools

import jax
import jax.numpy as jnp
from jax import lax
from jax.experimental import pallas as pl
from jax.experimental.pallas import tpu as pltpu
from jax.sharding import PartitionSpec as P

HEAD = 128
THETA = 10000
LOG2E = 1.4426950408889634
LOG2T = 13.287712379549449
HIDDEN = -2e30
VMEM = 60 * 2**20
MESH = pl.DeviceIdType.MESH
F32, BF16 = jnp.float32, jnp.bfloat16
scope = jax.named_scope


def _dot(a, b, ca=1, cb=0):
    return lax.dot_general(a, b, (((ca,), (cb,)), ((), ())), preferred_element_type=F32)


def _kernel(n, x_hbm, gain_hbm, wq_hbm, wk_hbm, wv_hbm, wo_hbm, out_ref,
            gain_s, xb, a, xr, wkv, wqb, wob, raw, q, kv, seen, acc, ys, top_s, mix_s, cos_s, sin_s,
            g_sem, x_sem, wkv_sem, wq_sem, wo_sem, a_send, a_recv, r_sem, r_send, r_recv,
            k_next, k_wrap, k_back, k_relay, k_edge, k_recv, s_send, s_recv, y_send, y_recv):
    own, d = x_hbm.shape
    toks = 2 * own
    nq, _, part = wqb.shape
    half = nq * part
    hk = kv.shape[1]
    kc = hk * HEAD
    group = q.shape[1] // toks
    me = lax.axis_index("sp")
    chip, core = lax.div(me, 2), lax.rem(me, 2)
    mate = {"sp": chip * 2 + 1 - core}

    def peer(at):
        return {"sp": at * 2 + core}

    mine = pl.multiple_of(core * own, own)
    theirs = pl.multiple_of((1 - core) * own, own)
    cols = pl.multiple_of(core * half, half)
    mate_cols = pl.multiple_of((1 - core) * half, half)

    barrier = pltpu.get_barrier_semaphore()
    pl.semaphore_signal(barrier, inc=1, device_id=mate, device_id_type=MESH)
    for i in range(1, n):
        pl.semaphore_signal(barrier, inc=1, device_id=peer(lax.rem(chip + i, n)), device_id_type=MESH)

    nx = x_sem.shape[0]
    rows = own // nx
    kcols = pl.ds(pl.multiple_of(core * kc, kc), kc)

    def x_copy(i):
        return pltpu.make_async_copy(x_hbm.at[pl.ds(i * rows, rows)], xb.at[pl.ds(i * rows, rows)], x_sem.at[i])

    def q_copy(i):
        return pltpu.make_async_copy(wq_hbm.at[:, pl.ds(pl.multiple_of(cols + i * part, part), part)], wqb.at[i], wq_sem.at[i])

    def o_copy(i):
        return pltpu.make_async_copy(wo_hbm.at[:, pl.ds(pl.multiple_of(cols + i * part, part), part)], wob.at[i], wo_sem.at[i])

    g_copy = pltpu.make_async_copy(gain_hbm, gain_s, g_sem)
    k_copy = pltpu.make_async_copy(wk_hbm.at[:, kcols], wkv.at[:, pl.ds(0, kc)], wkv_sem.at[0])
    v_copy = pltpu.make_async_copy(wv_hbm.at[:, kcols], wkv.at[:, pl.ds(kc, kc)], wkv_sem.at[1])
    r_copy = pltpu.make_async_copy(x_hbm.at[:, pl.ds(cols, half)], xr.at[pl.ds(mine, own)], r_sem)
    r_give = pltpu.make_async_remote_copy(x_hbm.at[:, pl.ds(mate_cols, half)], xr.at[pl.ds(mine, own)], r_send, r_recv, device_id=mate,
                                          device_id_type=MESH)
    g_copy.start()
    for i in range(nx):
        x_copy(i).start()
    k_copy.start()

    lane = lax.broadcasted_iota(jnp.int32, (toks, HEAD), 1)
    place = lax.broadcasted_iota(jnp.int32, (toks, HEAD), 0) + chip * toks
    turn = lax.rem(lane, HEAD // 2).astype(F32) * (-LOG2T / (HEAD // 2))
    angle = place.astype(F32) * jnp.exp2(turn)
    cos_s[...] = jnp.cos(angle)
    sin_s[...] = jnp.where(lane < HEAD // 2, -1.0, 1.0) * jnp.sin(angle)
    v_copy.start()

    def turned(t, cos, sin):
        t = t.astype(BF16).astype(F32)
        return (t * cos + pltpu.roll(t, HEAD // 2, 1) * sin).astype(BF16)

    def a_copy(i, at):
        here = pl.ds(pl.multiple_of(at + i * rows, rows), rows)
        return pltpu.make_async_remote_copy(a.at[here], a.at[here], a_send.at[i], a_recv.at[i], device_id=mate, device_id_type=MESH)

    g_copy.wait()
    gain = gain_s[...].astype(F32)[None]
    for i in range(nx):
        with scope("x_wait"):
            x_copy(i).wait()
        if i == 0:
            q_copy(0).start(priority=1)
        wide = xb[pl.ds(i * rows, rows), :].astype(F32)
        scale = lax.rsqrt(jnp.mean(wide * wide, -1, keepdims=True) + 1e-6)
        a[pl.ds(pl.multiple_of(mine + i * rows, rows), rows), :] = (wide * scale * gain).astype(BF16)
        if i == 0:
            with scope("barrier"):
                pl.semaphore_wait(barrier, n)
        a_copy(i, mine).start()

    def piece(sem, block, t, h, to):
        ref = kv.at[block, h, t]
        return pltpu.make_async_remote_copy(ref, ref, sem, k_recv.at[block, t, h], device_id=peer(to), device_id_type=MESH)

    last = n - 1
    sends, wraps, backs = chip < last, chip == 0, chip == 1
    relays, edges = (chip > 0) & (chip < last), (chip == 0) | (chip == last)
    edge_block, edge_to = jnp.where(chip == 0, 1, 0), jnp.where(chip == 0, last, last - 1)
    prev, nxt = lax.rem(chip + n - 1, n), lax.rem(chip + 1, n)

    def to_next(t, h):
        return piece(k_next.at[t, h], chip, t, h, nxt)

    def to_last(t, h):
        return piece(k_wrap.at[t, h], chip, t, h, last)

    def to_first(t):
        return piece(k_back.at[t], chip, t, 1, 0)

    def relay(t):
        return piece(k_relay.at[t], prev, t, 0, nxt)

    def edge(t):
        return piece(k_edge.at[t], edge_block, t, 1, edge_to)

    def arrived(block, t, h):
        piece(k_edge.at[t], block, t, h, chip).wait_recv()

    def when(flag, *copies):
        @pl.when(flag)
        def _():
            for copy in copies:
                copy.start()

    def keys_values(t):
        here = pl.ds(pl.multiple_of(t * own, own), own)
        r = _dot(a[here, :], wkv[...])
        cos, sin = cos_s[here, :], sin_s[here, :]
        for h in range(hk):
            kv[chip, h, t, 0] = turned(r[:, h * HEAD : (h + 1) * HEAD], cos, sin)
            kv[chip, h, t, 1] = r[:, kc + h * HEAD : kc + (h + 1) * HEAD].astype(BF16).T

    t0, t1 = core, 1 - core
    with scope("kv_wait"):
        k_copy.wait()
        v_copy.wait()
    q_copy(1).start(priority=1)

    def half_step(t):
        with scope("kv_mm"):
            keys_values(t)
        when(sends & (chip != last - 1), *(to_next(t, h) for h in range(hk)))
        when(chip == last - 1, *(to_next(t, h) for h in reversed(range(hk))))
        when(wraps, *(to_last(t, h) for h in reversed(range(hk))))
        when(backs, to_first(t))

    half_step(t0)

    def first_queries(at):
        here = pl.ds(at, own)
        raw[0, here, :] = _dot(a[here, :], wqb[0]).astype(BF16)

    with scope("q_wait"):
        q_copy(0).wait()
    q_copy(2).start(priority=1)
    with scope("q_own"):
        first_queries(mine)
    with scope("a_wait"):
        for j in range(nx):
            a_copy(j, theirs).wait_recv()
    half_step(t1)
    q_copy(3).start(priority=1)
    o_copy(0).start(priority=1)
    with scope("q_theirs"):
        first_queries(theirs)
    r_copy.start(priority=1)
    r_give.start()

    heads = part // HEAD

    def turn_queries(i):
        for j in range(heads):
            at = i * heads + j
            for t in range(2):
                here = slice(t * own, (t + 1) * own)
                q[at // group, pl.ds((t * group + at % group) * own, own), :] = turned(
                    raw[i % 2, here, j * HEAD : (j + 1) * HEAD], cos_s[here, :], sin_s[here, :])

    def relay_step(t):
        @pl.when(relays)
        def _():
            with scope("relay_wait"):
                arrived(prev, t, 0)
            relay(t).start()

    def edge_step(t, flag):
        @pl.when(flag)
        def _():
            with scope("edge_wait"):
                arrived(edge_block, t, 1)
            edge(t).start()

    for i in range(1, nq):
        with scope("q_wait"):
            q_copy(i).wait()
        o_copy(i).start(priority=1)
        with scope("q_mm"):
            raw[i % 2] = _dot(a[...], wqb[i]).astype(BF16)
            turn_queries(i - 1)
        if i == 1:
            relay_step(t0)
            edge_step(t0, wraps)
        if i == 2:
            relay_step(t1)
            edge_step(t1, wraps)
        if i == 2:
            edge_step(t0, chip == last)
        if i == 3:
            edge_step(t1, chip == last)
    turn_queries(nq - 1)

    e = HEAD**-0.5 * LOG2E
    strips = 4
    wide = q.shape[1] // strips
    some = wide // own

    def s_copy(h):
        here = pl.ds(h * group * HEAD, group * HEAD)
        return pltpu.make_async_remote_copy(seen.at[0, here], seen.at[1, here], s_send.at[h], s_recv.at[h], device_id=mate,
                                            device_id_type=MESH)

    def attend(h, blocks, first, final):
        ones = jnp.ones((8, 2 * own * len(blocks)), BF16)
        if first:
            ok = (lax.broadcasted_iota(jnp.int32, (own, wide), 1) & (own - 1)) >= lax.broadcasted_iota(jnp.int32, (own, wide), 0)

        def seen_by(s):
            t = s * 2 // strips
            return [(j, u) for n_j, j in enumerate(blocks) for u in range(2) if not first or n_j or u <= t], t

        def score(s):
            keys = jnp.concatenate([kv[j, h, u, 0] for j, u in seen_by(s)[0]], axis=0)
            return _dot(keys, q[h, pl.ds(s * wide, wide), :], 1, 1)

        scores, parts = {s: score(s) for s in range(2)}, {}

        def mix(s):
            at = pl.ds(s * wide, wide)
            p, keep = parts.pop(s)
            these, t = seen_by(s)
            values = jnp.concatenate([kv[j, h, u, 1] for j, u in these], axis=1)
            new = _dot(jnp.concatenate([values, ones[:, : values.shape[1]]], axis=0), p)
            if not first:
                new = mix_s[h, :, at] * keep + new
            if not final:
                mix_s[h, :, at] = new
                return
            o = (new[:HEAD] * (1 / new[HEAD : HEAD + 1])).astype(BF16)
            for i in range(some):
                row = pl.multiple_of((h * group + s % (strips // 2) * some + i) * HEAD, HEAD)
                seen[0, pl.ds(row, HEAD), t * own : (t + 1) * own] = o[:, i * own : (i + 1) * own]

        for s in range(strips):
            at = pl.ds(s * wide, wide)
            if s + 2 < strips:
                scores[s + 2] = score(s + 2)
            sc, keep, t = scores.pop(s), None, s * 2 // strips
            if first:
                here = jnp.where(ok, sc[t * own : (t + 1) * own], HIDDEN)
                sc = jnp.concatenate([x for x in (sc[: t * own], here, sc[(t + 1) * own :]) if x.shape[0]], axis=0)
            top = sc.max(axis=0, keepdims=True)
            if not first:
                old = top_s[h, :, at]
                top = jnp.maximum(old, top)
                keep = jnp.exp2((old - top) * e)
            if not final:
                top_s[h, :, at] = top
            parts[s] = jnp.exp2((sc - top) * e).astype(BF16), keep
            if s > 1:
                mix(s - 2)
        for s in range(strips - 2, strips):
            mix(s)
        if final:
            s_copy(h).start()

    def take(*pieces):
        with scope("arrive"):
            for block, h in pieces:
                for t in range(2):
                    arrived(block, t, h)

    def turn(i):
        return jnp.where(chip == last, hk - 1 - i, i)

    def near(i, _):
        h = turn(i)

        @pl.when(chip == 0)
        def _():
            with scope("att_1f"):
                attend(h, [chip], True, True)

        @pl.when((chip > 0) & jnp.logical_not(relays & (h == 0)))
        def _():
            take((prev, h))

        @pl.when(chip == 1)
        def _():
            with scope("att_2ff"):
                attend(h, [chip, prev], True, True)

        @pl.when(chip == 2)
        def _():
            with scope("att_2f"):
                attend(h, [chip, prev], True, False)

        @pl.when(chip == last)
        def _():
            @pl.when(h == 0)
            def _():
                take((0, h))

            with scope("att_3f"):
                attend(h, [chip, prev, 0], True, False)

    def far(i, _):
        h = turn(i)

        @pl.when(chip >= 2)
        def _():
            take((chip - 2, h))
            with scope("att_1"):
                attend(h, [chip - 2], False, True)

    lax.fori_loop(0, hk, near, None)
    lax.fori_loop(0, hk, far, None)

    def weight(i, side):
        return wob[i, pl.ds(side, half), :]

    def y_give(i, side):
        return pltpu.make_async_remote_copy(ys.at[pl.ds(theirs, own), pl.ds(i * part, part)],
                                            out_ref.at[:, pl.ds(pl.multiple_of(side + i * part, part), part)],
                                            y_send.at[i], y_recv.at[i], device_id=mate, device_id_type=MESH)

    def partial(i, c, rows_at):
        side = (cols, mate_cols)[c]
        return _dot(seen[c, :, rows_at], weight(i, side), 0, 0)

    with scope("r_wait"):
        r_copy.wait()
        r_give.wait_recv()
        for i in range(nq):
            o_copy(i).wait()
    every, it, me_at = slice(None), pl.ds(theirs, own), pl.ds(mine, own)
    for i in range(nq - 1):
        at = slice(i * part, (i + 1) * part)
        with scope("o_first"):
            acc[:, at] = xr[:, at].astype(F32) + partial(i, 0, every)
    with scope("seen_wait"):
        for h in range(hk):
            s_copy(h).wait_recv()
    for i in range(nq - 1):
        at = pl.ds(i * part, part)
        with scope("o_second"):
            ys[:, at] = (acc[:, at] + partial(i, 1, every)).astype(BF16)
        y_give(i, cols).start()
        out_ref[:, pl.ds(pl.multiple_of(cols + i * part, part), part)] = ys[me_at, at]
    at = pl.ds((nq - 1) * part, part)
    with scope("o_theirs"):
        ys[it, at] = (xr[it, at].astype(F32) + partial(nq - 1, 0, it) + partial(nq - 1, 1, it)).astype(BF16)
    y_give(nq - 1, cols).start()
    with scope("o_mine"):
        out_ref[:, pl.ds(pl.multiple_of(cols + (nq - 1) * part, part), part)] = (
            xr[me_at, at].astype(F32) + partial(nq - 1, 0, me_at) + partial(nq - 1, 1, me_at)).astype(BF16)

    with scope("y_wait"):
        for i in range(nq):
            y_give(i, cols).wait_send()
            y_give(i, mate_cols).wait_recv()
    for i in range(nx):
        a_copy(i, mine).wait_send()
    r_give.wait_send()
    for h in range(hk):
        s_copy(h).wait_send()

    def sent(flag, *copies):
        @pl.when(flag)
        def _():
            for copy in copies:
                copy.wait_send()

    both = [(t, h) for t in range(2) for h in range(hk)]
    sent(sends, *(to_next(t, h) for t, h in both))
    sent(wraps, *(to_last(t, h) for t, h in both))
    sent(backs, *(to_first(t) for t in range(2)))
    sent(relays, *(relay(t) for t in range(2)))
    sent(edges, *(edge(t) for t in range(2)))


def _call(x, gain, wq, wk, wv, wo, devices):
    own, d = x.shape
    n, toks = devices // 2, 2 * own
    half, kc = wq.shape[1] // 2, wk.shape[1] // 2
    nq, nx = 4, 4
    part = half // nq
    hk, group = kc // HEAD, half // kc
    cols = group * toks
    if (n, hk) != (4, 2):
        raise ValueError("group size")
    dma = pltpu.SemaphoreType.DMA
    any_ = pl.BlockSpec(memory_space=pltpu.HBM)
    return pl.pallas_call(
        functools.partial(_kernel, n),
        out_shape=pltpu.VMEM((own, d), BF16),
        in_specs=[any_] * 6,
        out_specs=pl.BlockSpec(memory_space=pltpu.VMEM),
        scratch_shapes=[
            pltpu.VMEM((d,), BF16),
            pltpu.VMEM((own, d), BF16),
            pltpu.VMEM((toks, d), BF16),
            pltpu.VMEM((toks, half), BF16),
            pltpu.VMEM((d, 2 * kc), BF16),
            pltpu.VMEM((nq, d, part), BF16),
            pltpu.VMEM((nq, d, part), BF16),
            pltpu.VMEM((2, toks, part), BF16),
            pltpu.VMEM((hk, cols, HEAD), BF16),
            pltpu.VMEM((n, hk, 2, 2, HEAD, HEAD), BF16),
            pltpu.VMEM((2, half, toks), BF16),
            pltpu.VMEM((toks, half), F32),
            pltpu.VMEM((toks, half), BF16),
            pltpu.VMEM((hk, 1, cols), F32),
            pltpu.VMEM((hk, HEAD + 8, cols), F32),
            pltpu.VMEM((toks, HEAD), F32),
            pltpu.VMEM((toks, HEAD), F32),
            dma, dma((nx,)), dma((2,)), dma((nq,)), dma((nq,)),
            dma((nx,)), dma((nx,)), dma, dma, dma,
            dma((2, hk)), dma((2, hk)), dma((2,)), dma((2,)), dma((2,)), dma((n, 2, hk)),
            dma((hk,)), dma((hk,)),
            dma((nq,)), dma((nq,)),
        ],
        compiler_params=pltpu.CompilerParams(collective_id=0, has_side_effects=True, vmem_limit_bytes=VMEM),
    )(x, gain, wq, wk, wv, wo)


def solution(mesh):
    devices = mesh.shape["sp"]

    def step(x, gain, wq, wk, wv, wo):
        return _call(x, gain, wq, wk, wv, wo, devices)

    tokens, whole = P(("dp", "sp"), None), P(None, None)
    return jax.shard_map(
        step,
        mesh=mesh,
        in_specs=(tokens, P(None), whole, whole, whole, whole),
        out_specs=tokens,
        check_vma=False,
    )
```

```python
import functools

import jax
import jax.numpy as jnp
from jax import lax
from jax.experimental import pallas as pl
from jax.experimental.pallas import tpu as pltpu
from jax.sharding import PartitionSpec as P

HEAD = 128
THETA = 10000
LOG2E = 1.4426950408889634
LOG2T = 13.287712379549449
HIDDEN = -2e30
VMEM = 60 * 2**20
MESH = pl.DeviceIdType.MESH
F32, BF16 = jnp.float32, jnp.bfloat16
scope = jax.named_scope


def _dot(a, b, ca=1, cb=0):
    return lax.dot_general(a, b, (((ca,), (cb,)), ((), ())), preferred_element_type=F32)


def _kernel(n, x_hbm, gain_hbm, wq_hbm, wk_hbm, wv_hbm, wo_hbm, out_ref,
            gain_s, xb, a, xr, wkv, wqb, wob, raw, q, kv, seen, acc, ys, top_s, mix_s, cos_s, sin_s,
            g_sem, x_sem, wkv_sem, wq_sem, wo_sem, a_send, a_recv, r_sem, r_send, r_recv,
            k_next, k_wrap, k_back, k_relay, k_edge, k_recv, s_send, s_recv, y_send, y_recv):
    own, d = x_hbm.shape
    toks = 2 * own
    nq, _, part = wqb.shape
    half = nq * part
    hk = kv.shape[1]
    kc = hk * HEAD
    group = q.shape[1] // toks
    me = lax.axis_index("sp")
    chip, core = lax.div(me, 2), lax.rem(me, 2)
    mate = {"sp": chip * 2 + 1 - core}

    def peer(at):
        return {"sp": at * 2 + core}

    mine = pl.multiple_of(core * own, own)
    theirs = pl.multiple_of((1 - core) * own, own)
    cols = pl.multiple_of(core * half, half)
    mate_cols = pl.multiple_of((1 - core) * half, half)

    nx = x_sem.shape[0]
    rows = own // nx
    kcols = pl.ds(pl.multiple_of(core * kc, kc), kc)

    def x_copy(i):
        return pltpu.make_async_copy(x_hbm.at[pl.ds(i * rows, rows)], xb.at[pl.ds(i * rows, rows)], x_sem.at[i])

    def q_copy(i):
        return pltpu.make_async_copy(wq_hbm.at[:, pl.ds(pl.multiple_of(cols + i * part, part), part)], wqb.at[i], wq_sem.at[i])

    def o_copy(i):
        return pltpu.make_async_copy(wo_hbm.at[:, pl.ds(pl.multiple_of(cols + i * part, part), part)], wob.at[i], wo_sem.at[i])

    for i in range(nx):
        x_copy(i).start()
    g_copy = pltpu.make_async_copy(gain_hbm, gain_s, g_sem)
    g_copy.start()
    barrier = pltpu.get_barrier_semaphore()
    pl.semaphore_signal(barrier, inc=1, device_id=mate, device_id_type=MESH)
    for i in range(1, n):
        pl.semaphore_signal(barrier, inc=1, device_id=peer(lax.rem(chip + i, n)), device_id_type=MESH)

    k_copy = pltpu.make_async_copy(wk_hbm.at[:, kcols], wkv.at[:, pl.ds(0, kc)], wkv_sem.at[0])
    v_copy = pltpu.make_async_copy(wv_hbm.at[:, kcols], wkv.at[:, pl.ds(kc, kc)], wkv_sem.at[1])
    r_copy = pltpu.make_async_copy(x_hbm.at[:, pl.ds(cols, half)], xr.at[pl.ds(mine, own)], r_sem)
    r_give = pltpu.make_async_remote_copy(x_hbm.at[:, pl.ds(mate_cols, half)], xr.at[pl.ds(mine, own)], r_send, r_recv, device_id=mate,
                                          device_id_type=MESH)
    k_copy.start()

    lane = lax.broadcasted_iota(jnp.int32, (toks, HEAD), 1)
    place = lax.broadcasted_iota(jnp.int32, (toks, HEAD), 0) + chip * toks
    turn = lax.rem(lane, HEAD // 2).astype(F32) * (-LOG2T / (HEAD // 2))
    angle = place.astype(F32) * jnp.exp2(turn)
    cos_s[...] = jnp.cos(angle)
    sin_s[...] = jnp.where(lane < HEAD // 2, -1.0, 1.0) * jnp.sin(angle)
    v_copy.start()

    def turned(t, cos, sin):
        t = t.astype(BF16).astype(F32)
        return (t * cos + pltpu.roll(t, HEAD // 2, 1) * sin).astype(BF16)

    def a_copy(i, at):
        here = pl.ds(pl.multiple_of(at + i * rows, rows), rows)
        return pltpu.make_async_remote_copy(a.at[here], a.at[here], a_send.at[i], a_recv.at[i], device_id=mate, device_id_type=MESH)

    for i in range(nx):
        with scope("x_wait"):
            x_copy(i).wait()
        if i == 0:
            q_copy(0).start(priority=1)
            with scope("g_wait"):
                g_copy.wait()
            gain = gain_s[...].astype(F32)[None]
        wide = xb[pl.ds(i * rows, rows), :].astype(F32)
        scale = lax.rsqrt(jnp.mean(wide * wide, -1, keepdims=True) + 1e-6)
        a[pl.ds(pl.multiple_of(mine + i * rows, rows), rows), :] = (wide * scale * gain).astype(BF16)
        if i == 0:
            with scope("barrier"):
                pl.semaphore_wait(barrier, n)
        a_copy(i, mine).start()

    def piece(sem, block, t, h, to, half=None):
        ref = kv.at[block, h, t] if half is None else kv.at[block, h, t, half]
        return pltpu.make_async_remote_copy(ref, ref, sem, k_recv.at[block, t, h], device_id=peer(to), device_id_type=MESH)

    t0, t1 = core, 1 - core
    last = n - 1
    sends, wraps, backs = chip < last, chip == 0, chip == 1
    relays, edges = (chip > 0) & (chip < last), (chip == 0) | (chip == last)
    edge_block, edge_to = jnp.where(chip == 0, 1, 0), jnp.where(chip == 0, last, last - 1)
    prev, nxt = lax.rem(chip + n - 1, n), lax.rem(chip + 1, n)

    def to_next(w, h):
        return piece(k_next.at[w, h], chip, t1 if w == 2 else t0, h, nxt, None if w == 2 else w)

    def to_last(w, h):
        return piece(k_wrap.at[w, h], chip, t1 if w == 2 else t0, h, last, None if w == 2 else w)

    def to_first(w):
        return piece(k_back.at[w], chip, t1 if w == 2 else t0, 1, 0, None if w == 2 else w)

    def relay(t):
        return piece(k_relay.at[t], prev, t, 0, nxt)

    def edge(t):
        return piece(k_edge.at[t], edge_block, t, 1, edge_to)

    def arrived(block, t, h):
        piece(k_edge.at[t], block, t, h, chip).wait_recv()

    def when(flag, *copies):
        @pl.when(flag)
        def _():
            for copy in copies:
                copy.start()

    def keys(r, t):
        here = pl.ds(pl.multiple_of(t * own, own), own)
        cos, sin = cos_s[here, :], sin_s[here, :]
        for h in range(hk):
            kv[chip, h, t, 0] = turned(r[:, h * HEAD : (h + 1) * HEAD], cos, sin)

    def values(r, t):
        for h in range(hk):
            kv[chip, h, t, 1] = r[:, h * HEAD : (h + 1) * HEAD].astype(BF16).T

    def send(w):
        when(sends, *(to_next(w, h) for h in range(hk)))
        when(wraps, *(to_last(w, h) for h in reversed(range(hk))))
        when(backs, to_first(w))

    with scope("k_wait"):
        k_copy.wait()
    with scope("k_mm"):
        keys(_dot(a[pl.ds(mine, own), :], wkv[:, :kc]), t0)
    send(0)
    with scope("v_wait"):
        v_copy.wait()
    q_copy(1).start(priority=1)
    with scope("v_mm"):
        values(_dot(a[pl.ds(mine, own), :], wkv[:, kc:]), t0)
    send(1)

    def first_queries(at):
        here = pl.ds(at, own)
        raw[0, here, :] = _dot(a[here, :], wqb[0]).astype(BF16)

    with scope("q_wait"):
        q_copy(0).wait()
    q_copy(2).start(priority=1)
    with scope("q_own"):
        first_queries(mine)
    with scope("a_wait"):
        for j in range(nx):
            a_copy(j, theirs).wait_recv()
    with scope("kv_mm"):
        r = _dot(a[pl.ds(theirs, own), :], wkv[...])
        keys(r[:, :kc], t1)
        values(r[:, kc:], t1)
    send(2)
    q_copy(3).start(priority=1)
    o_copy(0).start(priority=1)
    r_copy.start(priority=1)
    r_give.start()

    heads = part // HEAD

    def turn_queries(i):
        for j in range(heads):
            at = i * heads + j
            for t in range(2):
                here = slice(t * own, (t + 1) * own)
                q[at // group, pl.ds((t * group + at % group) * own, own), :] = turned(
                    raw[i, here, j * HEAD : (j + 1) * HEAD], cos_s[here, :], sin_s[here, :])

    def relay_step(t):
        @pl.when(relays)
        def _():
            with scope("relay_wait"):
                arrived(prev, t, 0)
            relay(t).start()

    def edge_step(t, flag):
        @pl.when(flag)
        def _():
            with scope("edge_wait"):
                arrived(edge_block, t, 1)
            edge(t).start()

    for i in range(1, nq):
        with scope("q_wait"):
            q_copy(i).wait()
        o_copy(i).start(priority=1)
        with scope("q_mm"):
            if i == 1:
                first_queries(theirs)
            raw[i] = _dot(a[...], wqb[i]).astype(BF16)
            turn_queries(i - 1)
        if i == 1:
            relay_step(t0)
            edge_step(t0, wraps)
        if i == 2:
            relay_step(t1)
            edge_step(t1, wraps)
        if i == 2:
            edge_step(t0, chip == last)
        if i == 3:
            edge_step(t1, chip == last)

    e = HEAD**-0.5 * LOG2E
    strips = 4
    wide = q.shape[1] // strips
    some = wide // own

    def s_copy(h):
        here = pl.ds(h * group * HEAD, group * HEAD)
        return pltpu.make_async_remote_copy(seen.at[0, here], seen.at[1, here], s_send.at[h], s_recv.at[h], device_id=mate,
                                            device_id_type=MESH)

    def attend(h, blocks, first, final):
        ones = jnp.ones((8, 2 * own * len(blocks)), BF16)
        if first:
            ok = (lax.broadcasted_iota(jnp.int32, (own, wide), 1) & (own - 1)) >= lax.broadcasted_iota(jnp.int32, (own, wide), 0)

        def seen_by(s):
            t = s * 2 // strips
            return [(j, u) for n_j, j in enumerate(blocks) for u in range(2) if not first or n_j or u <= t], t

        def score(s):
            keys = jnp.concatenate([kv[j, h, u, 0] for j, u in seen_by(s)[0]], axis=0)
            return _dot(keys, q[h, pl.ds(s * wide, wide), :], 1, 1)

        scores, parts = {s: score(s) for s in range(2)}, {}

        def mix(s):
            at = pl.ds(s * wide, wide)
            p, keep = parts.pop(s)
            these, t = seen_by(s)
            values = jnp.concatenate([kv[j, h, u, 1] for j, u in these], axis=1)
            new = _dot(jnp.concatenate([values, ones[:, : values.shape[1]]], axis=0), p)
            if not first:
                new = mix_s[h, :, at] * keep + new
            if not final:
                mix_s[h, :, at] = new
                return
            o = (new[:HEAD] * (1 / new[HEAD : HEAD + 1])).astype(BF16)
            for i in range(some):
                row = pl.multiple_of((h * group + s % (strips // 2) * some + i) * HEAD, HEAD)
                seen[0, pl.ds(row, HEAD), t * own : (t + 1) * own] = o[:, i * own : (i + 1) * own]

        for s in range(strips):
            at = pl.ds(s * wide, wide)
            if s + 2 < strips:
                scores[s + 2] = score(s + 2)
            sc, keep, t = scores.pop(s), None, s * 2 // strips
            if first:
                here = jnp.where(ok, sc[t * own : (t + 1) * own], HIDDEN)
                sc = jnp.concatenate([x for x in (sc[: t * own], here, sc[(t + 1) * own :]) if x.shape[0]], axis=0)
            top = sc.max(axis=0, keepdims=True)
            if not first:
                old = top_s[h, :, at]
                top = jnp.maximum(old, top)
                keep = jnp.exp2((old - top) * e)
            if not final:
                top_s[h, :, at] = top
            parts[s] = jnp.exp2((sc - top) * e).astype(BF16), keep
            if s > 1:
                mix(s - 2)
        for s in range(strips - 2, strips):
            mix(s)
        if final:
            s_copy(h).start()

    def take(*pieces):
        with scope("arrive"):
            for block, h in pieces:
                for t in range(2):
                    arrived(block, t, h)

    def near(h):
        def step(blocks, final):
            if h == 0:
                turn_queries(nq - 1)
            attend(h, blocks, True, final)

        @pl.when(chip > 1)
        def _():
            if h:
                take((prev, h))
            else:

                @pl.when(chip == last)
                def _():
                    take((prev, h))

            with scope("att_2f"):
                step([chip, prev], False)

        @pl.when(chip == 1)
        def _():
            if h:
                take((prev, h))
            with scope("att_2ff"):
                step([chip, prev], True)

        @pl.when(chip == 0)
        def _():
            with scope("att_1f"):
                step([chip], True)

    def far(h, _):
        @pl.when(chip == last)
        def _():
            @pl.when(h == 0)
            def _():
                take((0, h))

            take((1, h))
            with scope("att_2"):
                attend(h, [0, 1], False, True)

        @pl.when(chip == 2)
        def _():
            take((0, h))
            with scope("att_1"):
                attend(h, [0], False, True)

    for h in range(hk):
        near(h)
    lax.fori_loop(0, hk, far, None)

    def weight(i, side):
        return wob[i, pl.ds(side, half), :]

    def y_give(i, side):
        return pltpu.make_async_remote_copy(ys.at[pl.ds(theirs, own), pl.ds(i * part, part)],
                                            out_ref.at[:, pl.ds(pl.multiple_of(side + i * part, part), part)],
                                            y_send.at[i], y_recv.at[i], device_id=mate, device_id_type=MESH)

    def partial(i, c, rows_at):
        side = (cols, mate_cols)[c]
        return _dot(seen[c, :, rows_at], weight(i, side), 0, 0)

    with scope("r_wait"):
        r_copy.wait()
        r_give.wait_recv()
        for i in range(nq):
            o_copy(i).wait()
    every, it, me_at = slice(None), pl.ds(theirs, own), pl.ds(mine, own)
    for i in range(nq - 1):
        at = slice(i * part, (i + 1) * part)
        with scope("o_first"):
            acc[:, at] = xr[:, at].astype(F32) + partial(i, 0, every)
    with scope("seen_wait"):
        for h in range(hk):
            s_copy(h).wait_recv()
    with scope("o_second"):
        for i in range(nq - 1):
            at = slice(i * part, (i + 1) * part)
            ys[:, at] = (acc[:, at] + partial(i, 1, every)).astype(BF16)
    for i in range(nq - 1):
        y_give(i, cols).start()
    at = pl.ds((nq - 1) * part, part)
    with scope("o_theirs"):
        ys[it, at] = (xr[it, at].astype(F32) + partial(nq - 1, 0, it) + partial(nq - 1, 1, it)).astype(BF16)
    y_give(nq - 1, cols).start()
    with scope("o_mine"):
        out_ref[:, pl.ds(cols, half - part)] = ys[me_at, : half - part]
        out_ref[:, pl.ds(pl.multiple_of(cols + (nq - 1) * part, part), part)] = (
            xr[me_at, at].astype(F32) + partial(nq - 1, 0, me_at) + partial(nq - 1, 1, me_at)).astype(BF16)

    with scope("y_wait"):
        for i in range(nq):
            y_give(i, cols).wait_send()
            y_give(i, mate_cols).wait_recv()
    for i in range(nx):
        a_copy(i, mine).wait_send()
    r_give.wait_send()
    for h in range(hk):
        s_copy(h).wait_send()

    def sent(flag, *copies):
        @pl.when(flag)
        def _():
            for copy in copies:
                copy.wait_send()

    both = [(w, h) for w in range(3) for h in range(hk)]
    sent(sends, *(to_next(w, h) for w, h in both))
    sent(wraps, *(to_last(w, h) for w, h in both))
    sent(backs, *(to_first(w) for w in range(3)))
    sent(relays, *(relay(t) for t in range(2)))
    sent(edges, *(edge(t) for t in range(2)))


def _call(x, gain, wq, wk, wv, wo, devices):
    own, d = x.shape
    n, toks = devices // 2, 2 * own
    half, kc = wq.shape[1] // 2, wk.shape[1] // 2
    nq, nx = 4, 2
    part = half // nq
    hk, group = kc // HEAD, half // kc
    cols = group * toks
    if (n, hk) != (4, 2):
        raise ValueError("group size")
    dma = pltpu.SemaphoreType.DMA
    any_ = pl.BlockSpec(memory_space=pltpu.HBM)
    return pl.pallas_call(
        functools.partial(_kernel, n),
        out_shape=pltpu.VMEM((own, d), BF16),
        in_specs=[any_] * 6,
        out_specs=pl.BlockSpec(memory_space=pltpu.VMEM),
        scratch_shapes=[
            pltpu.VMEM((d,), BF16),
            pltpu.VMEM((own, d), BF16),
            pltpu.VMEM((toks, d), BF16),
            pltpu.VMEM((toks, half), BF16),
            pltpu.VMEM((d, 2 * kc), BF16),
            pltpu.VMEM((nq, d, part), BF16),
            pltpu.VMEM((nq, d, part), BF16),
            pltpu.VMEM((nq, toks, part), BF16),
            pltpu.VMEM((hk, cols, HEAD), BF16),
            pltpu.VMEM((n, hk, 2, 2, HEAD, HEAD), BF16),
            pltpu.VMEM((2, half, toks), BF16),
            pltpu.VMEM((toks, half), F32),
            pltpu.VMEM((toks, half), BF16),
            pltpu.VMEM((hk, 1, cols), F32),
            pltpu.VMEM((hk, HEAD + 8, cols), F32),
            pltpu.VMEM((toks, HEAD), F32),
            pltpu.VMEM((toks, HEAD), F32),
            dma, dma((nx,)), dma((2,)), dma((nq,)), dma((nq,)),
            dma((nx,)), dma((nx,)), dma, dma, dma,
            dma((3, hk)), dma((3, hk)), dma((3,)), dma((2,)), dma((2,)), dma((n, 2, hk)),
            dma((hk,)), dma((hk,)),
            dma((nq,)), dma((nq,)),
        ],
        compiler_params=pltpu.CompilerParams(collective_id=0, has_side_effects=True, vmem_limit_bytes=VMEM),
    )(x, gain, wq, wk, wv, wo)


def solution(mesh):
    devices = mesh.shape["sp"]

    def step(x, gain, wq, wk, wv, wo):
        return _call(x, gain, wq, wk, wv, wo, devices)

    tokens, whole = P(("dp", "sp"), None), P(None, None)
    return jax.shard_map(
        step,
        mesh=mesh,
        in_specs=(tokens, P(None), whole, whole, whole, whole),
        out_specs=tokens,
        check_vma=False,
    )
```

```python
import functools

import jax
import jax.numpy as jnp
from jax import lax
from jax.experimental import pallas as pl
from jax.experimental.pallas import tpu as pltpu
from jax.sharding import PartitionSpec as P

HEAD = 128
THETA = 10000
LOG2E = 1.4426950408889634
LOG2T = 13.287712379549449
HIDDEN = -2e30
VMEM = 60 * 2**20
MESH = pl.DeviceIdType.MESH
F32, BF16 = jnp.float32, jnp.bfloat16
scope = jax.named_scope


def _dot(a, b, ca=1, cb=0):
    return lax.dot_general(a, b, (((ca,), (cb,)), ((), ())), preferred_element_type=F32)


def _kernel(n, x_hbm, gain_hbm, wq_hbm, wk_hbm, wv_hbm, wo_hbm, out_ref,
            gain_s, xb, a, xr, wkv, wqb, wob, raw, q, kv, seen, acc, ys, top_s, mix_s, cos_s, sin_s,
            g_sem, x_sem, wkv_sem, wq_sem, wo_sem, a_send, a_recv, r_sem, r_send, r_recv,
            k_next, k_wrap, k_back, k_relay, k_edge, k_recv, s_send, s_recv, y_send, y_recv):
    own, d = x_hbm.shape
    toks = 2 * own
    nq, _, part = wqb.shape
    half = nq * part
    hk = kv.shape[1]
    kc = hk * HEAD
    group = q.shape[1] // toks
    me = lax.axis_index("sp")
    chip, core = lax.div(me, 2), lax.rem(me, 2)
    mate = {"sp": chip * 2 + 1 - core}

    def peer(at):
        return {"sp": at * 2 + core}

    mine = pl.multiple_of(core * own, own)
    theirs = pl.multiple_of((1 - core) * own, own)
    cols = pl.multiple_of(core * half, half)
    mate_cols = pl.multiple_of((1 - core) * half, half)

    nx = x_sem.shape[0]
    rows = own // nx
    kcols = pl.ds(pl.multiple_of(core * kc, kc), kc)

    def x_copy(i):
        return pltpu.make_async_copy(x_hbm.at[pl.ds(i * rows, rows)], xb.at[pl.ds(i * rows, rows)], x_sem.at[i])

    def q_copy(i):
        return pltpu.make_async_copy(wq_hbm.at[:, pl.ds(pl.multiple_of(cols + i * part, part), part)], wqb.at[i], wq_sem.at[i])

    def o_copy(i):
        return pltpu.make_async_copy(wo_hbm.at[:, pl.ds(pl.multiple_of(cols + i * part, part), part)], wob.at[i], wo_sem.at[i])

    for i in range(nx):
        x_copy(i).start()
    g_copy = pltpu.make_async_copy(gain_hbm, gain_s, g_sem)
    g_copy.start()
    barrier = pltpu.get_barrier_semaphore()
    pl.semaphore_signal(barrier, inc=1, device_id=mate, device_id_type=MESH)
    for i in range(1, n):
        pl.semaphore_signal(barrier, inc=1, device_id=peer(lax.rem(chip + i, n)), device_id_type=MESH)

    k_copy = pltpu.make_async_copy(wk_hbm.at[:, kcols], wkv.at[:, pl.ds(0, kc)], wkv_sem.at[0])
    v_copy = pltpu.make_async_copy(wv_hbm.at[:, kcols], wkv.at[:, pl.ds(kc, kc)], wkv_sem.at[1])
    r_copy = pltpu.make_async_copy(x_hbm.at[:, pl.ds(cols, half)], xr.at[pl.ds(mine, own)], r_sem)
    r_give = pltpu.make_async_remote_copy(x_hbm.at[:, pl.ds(mate_cols, half)], xr.at[pl.ds(mine, own)], r_send, r_recv, device_id=mate,
                                          device_id_type=MESH)
    k_copy.start()

    lane = lax.broadcasted_iota(jnp.int32, (toks, HEAD), 1)
    place = lax.broadcasted_iota(jnp.int32, (toks, HEAD), 0) + chip * toks
    turn = lax.rem(lane, HEAD // 2).astype(F32) * (-LOG2T / (HEAD // 2))
    angle = place.astype(F32) * jnp.exp2(turn)
    cos_s[...] = jnp.cos(angle)
    sin_s[...] = jnp.where(lane < HEAD // 2, -1.0, 1.0) * jnp.sin(angle)
    v_copy.start()

    def turned(t, cos, sin):
        t = t.astype(BF16).astype(F32)
        return (t * cos + pltpu.roll(t, HEAD // 2, 1) * sin).astype(BF16)

    def a_copy(i, at):
        here = pl.ds(pl.multiple_of(at + i * rows, rows), rows)
        return pltpu.make_async_remote_copy(a.at[here], a.at[here], a_send.at[i], a_recv.at[i], device_id=mate, device_id_type=MESH)

    for i in range(nx):
        with scope("x_wait"):
            x_copy(i).wait()
        if i == 0:
            q_copy(0).start(priority=1)
            with scope("g_wait"):
                g_copy.wait()
            gain = gain_s[...].astype(F32)[None]
        wide = xb[pl.ds(i * rows, rows), :].astype(F32)
        scale = lax.rsqrt(jnp.mean(wide * wide, -1, keepdims=True) + 1e-6)
        a[pl.ds(pl.multiple_of(mine + i * rows, rows), rows), :] = (wide * scale * gain).astype(BF16)
        if i == 0:
            with scope("barrier"):
                pl.semaphore_wait(barrier, n)
        a_copy(i, mine).start()

    def piece(sem, block, t, h, to, half=None):
        ref = kv.at[block, h, t] if half is None else kv.at[block, h, t, half]
        return pltpu.make_async_remote_copy(ref, ref, sem, k_recv.at[block, t, h], device_id=peer(to), device_id_type=MESH)

    t0, t1 = core, 1 - core
    last = n - 1
    sends, wraps, backs = chip < last, chip == 0, chip == 1
    relays, edges = (chip > 0) & (chip < last), (chip == 0) | (chip == last)
    edge_block, edge_to = jnp.where(chip == 0, 1, 0), jnp.where(chip == 0, last, last - 1)
    prev, nxt = lax.rem(chip + n - 1, n), lax.rem(chip + 1, n)

    def to_next(w, h):
        return piece(k_next.at[w, h], chip, t1 if w == 2 else t0, h, nxt, None if w == 2 else w)

    def to_last(w, h):
        return piece(k_wrap.at[w, h], chip, t1 if w == 2 else t0, h, last, None if w == 2 else w)

    def to_first(w):
        return piece(k_back.at[w], chip, t1 if w == 2 else t0, 1, 0, None if w == 2 else w)

    def relay(t):
        return piece(k_relay.at[t], prev, t, 0, nxt)

    def edge(t):
        return piece(k_edge.at[t], edge_block, t, 1, edge_to)

    def arrived(block, t, h):
        piece(k_edge.at[t], block, t, h, chip).wait_recv()

    def when(flag, *copies):
        @pl.when(flag)
        def _():
            for copy in copies:
                copy.start()

    def keys(r, t):
        here = pl.ds(pl.multiple_of(t * own, own), own)
        cos, sin = cos_s[here, :], sin_s[here, :]
        for h in range(hk):
            kv[chip, h, t, 0] = turned(r[:, h * HEAD : (h + 1) * HEAD], cos, sin)

    def values(r, t):
        for h in range(hk):
            kv[chip, h, t, 1] = r[:, h * HEAD : (h + 1) * HEAD].astype(BF16).T

    def send(w):
        when(sends, *(to_next(w, h) for h in range(hk)))
        when(wraps, *(to_last(w, h) for h in reversed(range(hk))))
        when(backs, to_first(w))

    def own_product(columns):
        rows_at, mid = pl.ds(mine, own), d // 2
        return _dot(a[rows_at, :mid], wkv[:mid, columns]) + _dot(a[rows_at, mid:], wkv[mid:, columns])

    with scope("k_wait"):
        k_copy.wait()
    with scope("k_mm"):
        keys(own_product(slice(0, kc)), t0)
    send(0)
    with scope("v_wait"):
        v_copy.wait()
    q_copy(1).start(priority=1)
    with scope("v_mm"):
        values(own_product(slice(kc, 2 * kc)), t0)
    send(1)

    def first_queries(at):
        here = pl.ds(at, own)
        raw[0, here, :] = _dot(a[here, :], wqb[0]).astype(BF16)

    def others():
        with scope("a_wait"):
            for j in range(nx):
                a_copy(j, theirs).wait_recv()
        with scope("kv_mm"):
            r = _dot(a[pl.ds(theirs, own), :], wkv[...])
            keys(r[:, :kc], t1)
            values(r[:, kc:], t1)
        send(2)

    def first_weights():
        with scope("q_wait"):
            q_copy(0).wait()
        q_copy(2).start(priority=1)

    def second_weights():
        q_copy(3).start(priority=1)
        with scope("q_wait"):
            q_copy(1).wait()
        o_copy(0).start(priority=1)

    heads = part // HEAD

    def turn_queries(i):
        for j in range(heads):
            at = i * heads + j
            for t in range(2):
                here = slice(t * own, (t + 1) * own)
                q[at // group, pl.ds((t * group + at % group) * own, own), :] = turned(
                    raw[i, here, j * HEAD : (j + 1) * HEAD], cos_s[here, :], sin_s[here, :])

    def relay_step(t):
        @pl.when(relays)
        def _():
            with scope("relay_wait"):
                arrived(prev, t, 0)
            relay(t).start()

    def edge_step(t, flag):
        @pl.when(flag)
        def _():
            with scope("edge_wait"):
                arrived(edge_block, t, 1)
            edge(t).start()

    @pl.when(core == 0)
    def _():
        others()
        first_weights()
        with scope("q_mm"):
            raw[0] = _dot(a[...], wqb[0]).astype(BF16)
        second_weights()
        with scope("q_mm"):
            raw[1] = _dot(a[...], wqb[1]).astype(BF16)
            turn_queries(0)

    @pl.when(core == 1)
    def _():
        first_weights()
        with scope("q_own"):
            first_queries(mine)
        others()
        second_weights()
        with scope("q_mm"):
            first_queries(theirs)
            raw[1] = _dot(a[...], wqb[1]).astype(BF16)
            turn_queries(0)

    r_copy.start(priority=1)
    r_give.start()
    for i in range(1, nq):
        if i > 1:
            with scope("q_wait"):
                q_copy(i).wait()
            o_copy(i).start(priority=1)
            with scope("q_mm"):
                raw[i] = _dot(a[...], wqb[i]).astype(BF16)
                turn_queries(i - 1)
        else:
            o_copy(i).start(priority=1)
        if i == 1:
            relay_step(t0)
            edge_step(t0, wraps)
        if i == 2:
            relay_step(t1)
            edge_step(t1, wraps)
        if i == 2:
            edge_step(t0, chip == last)
        if i == 3:
            edge_step(t1, chip == last)

    e = HEAD**-0.5 * LOG2E
    strips = 4
    wide = q.shape[1] // strips
    some = wide // own

    def s_copy(h):
        here = pl.ds(h * group * HEAD, group * HEAD)
        return pltpu.make_async_remote_copy(seen.at[0, here], seen.at[1, here], s_send.at[h], s_recv.at[h], device_id=mate,
                                            device_id_type=MESH)

    def attend(h, blocks, first, final):
        ones = jnp.ones((8, 2 * own * len(blocks)), BF16)
        if first:
            ok = (lax.broadcasted_iota(jnp.int32, (own, wide), 1) & (own - 1)) >= lax.broadcasted_iota(jnp.int32, (own, wide), 0)

        def seen_by(s):
            t = s * 2 // strips
            return [(j, u) for n_j, j in enumerate(blocks) for u in range(2) if not first or n_j or u <= t], t

        def score(s):
            keys = jnp.concatenate([kv[j, h, u, 0] for j, u in seen_by(s)[0]], axis=0)
            return _dot(keys, q[h, pl.ds(s * wide, wide), :], 1, 1)

        scores, parts = {s: score(s) for s in range(2)}, {}

        def mix(s):
            at = pl.ds(s * wide, wide)
            p, keep = parts.pop(s)
            these, t = seen_by(s)
            values = jnp.concatenate([kv[j, h, u, 1] for j, u in these], axis=1)
            new = _dot(jnp.concatenate([values, ones[:, : values.shape[1]]], axis=0), p)
            if not first:
                new = mix_s[h, :, at] * keep + new
            if not final:
                mix_s[h, :, at] = new
                return
            o = (new[:HEAD] * (1 / new[HEAD : HEAD + 1])).astype(BF16)
            for i in range(some):
                row = pl.multiple_of((h * group + s % (strips // 2) * some + i) * HEAD, HEAD)
                seen[0, pl.ds(row, HEAD), t * own : (t + 1) * own] = o[:, i * own : (i + 1) * own]

        for s in range(strips):
            at = pl.ds(s * wide, wide)
            if s + 2 < strips:
                scores[s + 2] = score(s + 2)
            sc, keep, t = scores.pop(s), None, s * 2 // strips
            if first:
                here = jnp.where(ok, sc[t * own : (t + 1) * own], HIDDEN)
                sc = jnp.concatenate([x for x in (sc[: t * own], here, sc[(t + 1) * own :]) if x.shape[0]], axis=0)
            top = sc.max(axis=0, keepdims=True)
            if not first:
                old = top_s[h, :, at]
                top = jnp.maximum(old, top)
                keep = jnp.exp2((old - top) * e)
            if not final:
                top_s[h, :, at] = top
            parts[s] = jnp.exp2((sc - top) * e).astype(BF16), keep
            if s > 1:
                mix(s - 2)
        for s in range(strips - 2, strips):
            mix(s)
        if final:
            s_copy(h).start()

    def take(*pieces):
        with scope("arrive"):
            for block, h in pieces:
                for t in range(2):
                    arrived(block, t, h)

    def near(h):
        if h:
            take((prev, h))
        else:

            @pl.when(chip == last)
            def _():
                take((prev, h))

        with scope("att_2f"):
            if h == 0:
                turn_queries(nq - 1)
            attend(h, [chip, prev], True, False)

    def only(h, _):
        @pl.when(chip == 1)
        def _():
            @pl.when(h > 0)
            def _():
                take((prev, h))

            with scope("att_2ff"):
                attend(h, [chip, prev], True, True)

        @pl.when(chip == 0)
        def _():
            with scope("att_1f"):
                attend(h, [chip], True, True)

    def far(h, _):
        @pl.when(chip == last)
        def _():
            @pl.when(h == 0)
            def _():
                take((0, h))

            take((1, h))
            with scope("att_2"):
                attend(h, [0, 1], False, True)

        @pl.when(chip == 2)
        def _():
            take((0, h))
            with scope("att_1"):
                attend(h, [0], False, True)

    @pl.when(chip > 1)
    def _():
        for h in range(hk):
            near(h)
        lax.fori_loop(0, hk, far, None)

    @pl.when(chip < 2)
    def _():
        turn_queries(nq - 1)
        lax.fori_loop(0, hk, only, None)

    def weight(i, side):
        return wob[i, pl.ds(side, half), :]

    def y_give(i, side):
        return pltpu.make_async_remote_copy(ys.at[pl.ds(theirs, own), pl.ds(i * part, part)],
                                            out_ref.at[:, pl.ds(pl.multiple_of(side + i * part, part), part)],
                                            y_send.at[i], y_recv.at[i], device_id=mate, device_id_type=MESH)

    def partial(i, c, rows_at):
        side = (cols, mate_cols)[c]
        return _dot(seen[c, :, rows_at], weight(i, side), 0, 0)

    with scope("r_wait"):
        r_copy.wait()
        r_give.wait_recv()
        for i in range(nq):
            o_copy(i).wait()
    every, it, me_at = slice(None), pl.ds(theirs, own), pl.ds(mine, own)
    for i in range(nq - 1):
        at = slice(i * part, (i + 1) * part)
        with scope("o_first"):
            acc[:, at] = xr[:, at].astype(F32) + partial(i, 0, every)
    with scope("seen_wait"):
        for h in range(hk):
            s_copy(h).wait_recv()
    with scope("o_second"):
        for i in range(nq - 1):
            at = slice(i * part, (i + 1) * part)
            ys[:, at] = (acc[:, at] + partial(i, 1, every)).astype(BF16)
    for i in range(nq - 1):
        y_give(i, cols).start()
    at = pl.ds((nq - 1) * part, part)
    with scope("o_theirs"):
        ys[it, at] = (xr[it, at].astype(F32) + partial(nq - 1, 0, it) + partial(nq - 1, 1, it)).astype(BF16)
    y_give(nq - 1, cols).start()
    with scope("o_mine"):
        out_ref[:, pl.ds(cols, half - part)] = ys[me_at, : half - part]
        out_ref[:, pl.ds(pl.multiple_of(cols + (nq - 1) * part, part), part)] = (
            xr[me_at, at].astype(F32) + partial(nq - 1, 0, me_at) + partial(nq - 1, 1, me_at)).astype(BF16)

    with scope("y_wait"):
        for i in range(nq):
            y_give(i, cols).wait_send()
            y_give(i, mate_cols).wait_recv()
    for i in range(nx):
        a_copy(i, mine).wait_send()
    r_give.wait_send()
    for h in range(hk):
        s_copy(h).wait_send()

    def sent(flag, *copies):
        @pl.when(flag)
        def _():
            for copy in copies:
                copy.wait_send()

    both = [(w, h) for w in range(3) for h in range(hk)]
    sent(sends, *(to_next(w, h) for w, h in both))
    sent(wraps, *(to_last(w, h) for w, h in both))
    sent(backs, *(to_first(w) for w in range(3)))
    sent(relays, *(relay(t) for t in range(2)))
    sent(edges, *(edge(t) for t in range(2)))


def _call(x, gain, wq, wk, wv, wo, devices):
    own, d = x.shape
    n, toks = devices // 2, 2 * own
    half, kc = wq.shape[1] // 2, wk.shape[1] // 2
    nq, nx = 4, 2
    part = half // nq
    hk, group = kc // HEAD, half // kc
    cols = group * toks
    if (n, hk) != (4, 2):
        raise ValueError("group size")
    dma = pltpu.SemaphoreType.DMA
    any_ = pl.BlockSpec(memory_space=pltpu.HBM)
    return pl.pallas_call(
        functools.partial(_kernel, n),
        out_shape=pltpu.VMEM((own, d), BF16),
        in_specs=[any_] * 6,
        out_specs=pl.BlockSpec(memory_space=pltpu.VMEM),
        scratch_shapes=[
            pltpu.VMEM((d,), BF16),
            pltpu.VMEM((own, d), BF16),
            pltpu.VMEM((toks, d), BF16),
            pltpu.VMEM((toks, half), BF16),
            pltpu.VMEM((d, 2 * kc), BF16),
            pltpu.VMEM((nq, d, part), BF16),
            pltpu.VMEM((nq, d, part), BF16),
            pltpu.VMEM((nq, toks, part), BF16),
            pltpu.VMEM((hk, cols, HEAD), BF16),
            pltpu.VMEM((n, hk, 2, 2, HEAD, HEAD), BF16),
            pltpu.VMEM((2, half, toks), BF16),
            pltpu.VMEM((toks, half), F32),
            pltpu.VMEM((toks, half), BF16),
            pltpu.VMEM((hk, 1, cols), F32),
            pltpu.VMEM((hk, HEAD + 8, cols), F32),
            pltpu.VMEM((toks, HEAD), F32),
            pltpu.VMEM((toks, HEAD), F32),
            dma, dma((nx,)), dma((2,)), dma((nq,)), dma((nq,)),
            dma((nx,)), dma((nx,)), dma, dma, dma,
            dma((3, hk)), dma((3, hk)), dma((3,)), dma((2,)), dma((2,)), dma((n, 2, hk)),
            dma((hk,)), dma((hk,)),
            dma((nq,)), dma((nq,)),
        ],
        compiler_params=pltpu.CompilerParams(collective_id=0, has_side_effects=True, vmem_limit_bytes=VMEM),
    )(x, gain, wq, wk, wv, wo)


def solution(mesh):
    devices = mesh.shape["sp"]

    def step(x, gain, wq, wk, wv, wo):
        return _call(x, gain, wq, wk, wv, wo, devices)

    tokens, whole = P(("dp", "sp"), None), P(None, None)
    return jax.shard_map(
        step,
        mesh=mesh,
        in_specs=(tokens, P(None), whole, whole, whole, whole),
        out_specs=tokens,
        check_vma=False,
    )
```

```python
import functools

import jax
import jax.numpy as jnp
from jax import lax
from jax.experimental import pallas as pl
from jax.experimental.pallas import tpu as pltpu
from jax.sharding import PartitionSpec as P

HEAD = 128
THETA = 10000
LOG2E = 1.4426950408889634
LOG2T = 13.287712379549449
HIDDEN = -2e30
VMEM = 60 * 2**20
MESH = pl.DeviceIdType.MESH
F32, BF16 = jnp.float32, jnp.bfloat16
scope = jax.named_scope


def _dot(a, b, ca=1, cb=0):
    return lax.dot_general(a, b, (((ca,), (cb,)), ((), ())), preferred_element_type=F32)


def _kernel(n, x_hbm, gain_hbm, wq_hbm, wk_hbm, wv_hbm, wo_hbm, out_ref,
            gain_s, xb, a, xr, wkv, wqb, wob, raw, q, kv, seen, acc, ys, top_s, mix_s, cos_s, sin_s,
            g_sem, x_sem, wkv_sem, wq_sem, wo_sem, a_send, a_recv, r_sem, r_send, r_recv,
            k_next, k_wrap, k_back, k_relay, k_edge, k_recv, s_send, s_recv, y_send, y_recv):
    own, d = x_hbm.shape
    toks = 2 * own
    nq, _, part = wqb.shape
    half = nq * part
    hk = kv.shape[1]
    kc = hk * HEAD
    group = q.shape[1] // toks
    me = lax.axis_index("sp")
    chip, core = lax.div(me, 2), lax.rem(me, 2)
    mate = {"sp": chip * 2 + 1 - core}

    def peer(at):
        return {"sp": at * 2 + core}

    mine = pl.multiple_of(core * own, own)
    theirs = pl.multiple_of((1 - core) * own, own)
    cols = pl.multiple_of(core * half, half)
    mate_cols = pl.multiple_of((1 - core) * half, half)

    nx = x_sem.shape[0]
    rows = own // nx
    kcols = pl.ds(pl.multiple_of(core * kc, kc), kc)

    def x_copy(i):
        return pltpu.make_async_copy(x_hbm.at[pl.ds(i * rows, rows)], xb.at[pl.ds(i * rows, rows)], x_sem.at[i])

    def q_copy(i):
        return pltpu.make_async_copy(wq_hbm.at[:, pl.ds(pl.multiple_of(cols + i * part, part), part)], wqb.at[i], wq_sem.at[i])

    def o_copy(i):
        return pltpu.make_async_copy(wo_hbm.at[:, pl.ds(pl.multiple_of(cols + i * part, part), part)], wob.at[i], wo_sem.at[i])

    for i in range(nx):
        x_copy(i).start()
    g_copy = pltpu.make_async_copy(gain_hbm, gain_s, g_sem)
    g_copy.start()
    barrier = pltpu.get_barrier_semaphore()
    pl.semaphore_signal(barrier, inc=1, device_id=mate, device_id_type=MESH)
    for i in range(1, n):
        pl.semaphore_signal(barrier, inc=1, device_id=peer(lax.rem(chip + i, n)), device_id_type=MESH)

    k_copy = pltpu.make_async_copy(wk_hbm.at[:, kcols], wkv.at[:, pl.ds(0, kc)], wkv_sem.at[0])
    v_copy = pltpu.make_async_copy(wv_hbm.at[:, kcols], wkv.at[:, pl.ds(kc, kc)], wkv_sem.at[1])
    r_copy = pltpu.make_async_copy(x_hbm.at[:, pl.ds(cols, half)], xr.at[pl.ds(mine, own)], r_sem)
    r_give = pltpu.make_async_remote_copy(x_hbm.at[:, pl.ds(mate_cols, half)], xr.at[pl.ds(mine, own)], r_send, r_recv, device_id=mate,
                                          device_id_type=MESH)
    k_copy.start()

    lane = lax.broadcasted_iota(jnp.int32, (toks, HEAD), 1)
    place = lax.broadcasted_iota(jnp.int32, (toks, HEAD), 0) + chip * toks
    turn = lax.rem(lane, HEAD // 2).astype(F32) * (-LOG2T / (HEAD // 2))
    angle = place.astype(F32) * jnp.exp2(turn)
    cos_s[...] = jnp.cos(angle)
    sin_s[...] = jnp.where(lane < HEAD // 2, -1.0, 1.0) * jnp.sin(angle)
    v_copy.start()

    def turned(t, cos, sin):
        t = t.astype(BF16).astype(F32)
        return (t * cos + pltpu.roll(t, HEAD // 2, 1) * sin).astype(BF16)

    def early(i):
        @pl.when(chip == 0)
        def _():
            for j in range(i + 1, nq):
                q_copy(j).start(priority=1)

    def in_turn(i):
        @pl.when(chip > 0)
        def _():
            q_copy(i).start(priority=1)

    def a_copy(i, at):
        here = pl.ds(pl.multiple_of(at + i * rows, rows), rows)
        return pltpu.make_async_remote_copy(a.at[here], a.at[here], a_send.at[i], a_recv.at[i], device_id=mate, device_id_type=MESH)

    for i in range(nx):
        with scope("x_wait"):
            x_copy(i).wait()
        if i == 0:
            q_copy(0).start(priority=1)
            early(0)
            with scope("g_wait"):
                g_copy.wait()
            gain = gain_s[...].astype(F32)[None]
        wide = xb[pl.ds(i * rows, rows), :].astype(F32)
        scale = lax.rsqrt(jnp.mean(wide * wide, -1, keepdims=True) + 1e-6)
        a[pl.ds(pl.multiple_of(mine + i * rows, rows), rows), :] = (wide * scale * gain).astype(BF16)
        if i == 0:
            with scope("barrier"):
                pl.semaphore_wait(barrier, n)
        a_copy(i, mine).start()

    def piece(sem, block, t, h, to, half=None):
        ref = kv.at[block, h, t] if half is None else kv.at[block, h, t, half]
        return pltpu.make_async_remote_copy(ref, ref, sem, k_recv.at[block, t, h], device_id=peer(to), device_id_type=MESH)

    t0, t1 = core, 1 - core
    last = n - 1
    sends, wraps, backs = chip < last, chip == 0, chip == 1
    relays, edges = (chip > 0) & (chip < last), (chip == 0) | (chip == last)
    edge_block, edge_to = jnp.where(chip == 0, 1, 0), jnp.where(chip == 0, last, last - 1)
    prev, nxt = lax.rem(chip + n - 1, n), lax.rem(chip + 1, n)

    def to_next(w, h):
        return piece(k_next.at[w, h], chip, t1 if w == 2 else t0, h, nxt, None if w == 2 else w)

    def to_last(w, h):
        return piece(k_wrap.at[w, h], chip, t1 if w == 2 else t0, h, last, None if w == 2 else w)

    def to_first(w):
        return piece(k_back.at[w], chip, t1 if w == 2 else t0, 0 if w == 2 else 1, 0, None if w == 2 else w)

    def relay_head(i):
        return jnp.where(chip == 1, 0, i)

    def relay(i):
        return piece(k_relay.at[i], prev, (t0, t1)[i], relay_head(i), nxt)

    def edge_head(i):
        return jnp.where(chip == 0, 1 - i, 1)

    def edge(i):
        return piece(k_edge.at[i], edge_block, (t0, t1)[i], edge_head(i), edge_to)

    def arrived(block, t, h):
        piece(k_edge.at[0], block, t, h, chip).wait_recv()

    def when(flag, *copies):
        @pl.when(flag)
        def _():
            for copy in copies:
                copy.start()

    def keys(r, t):
        here = pl.ds(pl.multiple_of(t * own, own), own)
        cos, sin = cos_s[here, :], sin_s[here, :]
        for h in range(hk):
            kv[chip, h, t, 0] = turned(r[:, h * HEAD : (h + 1) * HEAD], cos, sin)

    def values(r, t):
        for h in range(hk):
            kv[chip, h, t, 1] = r[:, h * HEAD : (h + 1) * HEAD].astype(BF16).T

    def send(w):
        when(sends, *(to_next(w, h) for h in range(hk)))
        when(wraps, *(to_last(w, h) for h in reversed(range(hk))))
        when(backs, to_first(w))

    def own_product(columns):
        rows_at, mid = pl.ds(mine, own), d // 2
        return _dot(a[rows_at, :mid], wkv[:mid, columns]) + _dot(a[rows_at, mid:], wkv[mid:, columns])

    with scope("k_wait"):
        k_copy.wait()
    with scope("k_mm"):
        keys(own_product(slice(0, kc)), t0)
    send(0)
    with scope("v_wait"):
        v_copy.wait()
    in_turn(1)
    with scope("v_mm"):
        values(own_product(slice(kc, 2 * kc)), t0)
    send(1)

    def first_queries(at):
        here = pl.ds(at, own)
        raw[0, here, :] = _dot(a[here, :], wqb[0]).astype(BF16)

    def others():
        with scope("a_wait"):
            for j in range(nx):
                a_copy(j, theirs).wait_recv()
        with scope("kv_mm"):
            r = _dot(a[pl.ds(theirs, own), :], wkv[...])
            keys(r[:, :kc], t1)
            values(r[:, kc:], t1)
        send(2)

    def first_weights():
        with scope("q_wait"):
            q_copy(0).wait()
        in_turn(2)

    def second_weights():
        in_turn(3)
        with scope("q_wait"):
            q_copy(1).wait()
        o_copy(0).start(priority=1)

    heads = part // HEAD

    def turn_queries(i):
        for j in range(heads):
            at = i * heads + j
            for t in range(2):
                here = slice(t * own, (t + 1) * own)
                q[at // group, pl.ds((t * group + at % group) * own, own), :] = turned(
                    raw[i, here, j * HEAD : (j + 1) * HEAD], cos_s[here, :], sin_s[here, :])

    def relay_step(i, flag):
        @pl.when(flag)
        def _():
            with scope("relay_wait"):
                arrived(prev, (t0, t1)[i], relay_head(i))
            relay(i).start()

    def edge_step(i, flag):
        @pl.when(flag)
        def _():
            with scope("edge_wait"):
                arrived(edge_block, (t0, t1)[i], edge_head(i))
            edge(i).start()

    @pl.when(core == 0)
    def _():
        others()
        first_weights()
        with scope("q_mm"):
            raw[0] = _dot(a[...], wqb[0]).astype(BF16)
        second_weights()
        with scope("q_mm"):
            raw[1] = _dot(a[...], wqb[1]).astype(BF16)
            turn_queries(0)

    @pl.when(core == 1)
    def _():
        first_weights()
        with scope("q_own"):
            first_queries(mine)
        others()
        second_weights()
        with scope("q_mm"):
            first_queries(theirs)
            raw[1] = _dot(a[...], wqb[1]).astype(BF16)
            turn_queries(0)

    r_copy.start(priority=1)
    r_give.start()
    for i in range(1, nq):
        if i > 1:
            with scope("q_wait"):
                q_copy(i).wait()
            if i + 1 < nq:
                o_copy(i + 1).start(priority=1)
            with scope("q_mm"):
                raw[i] = _dot(a[...], wqb[i]).astype(BF16)
                turn_queries(i - 1)
        else:
            o_copy(1).start(priority=1)
            o_copy(2).start(priority=1)
        if i == 1:
            relay_step(0, relays)
            edge_step(1, wraps)
        if i == 2:
            relay_step(1, chip == 1)
            edge_step(0, edges)
        if i == 3:
            relay_step(1, chip == 2)
            edge_step(1, chip == last)

    e = HEAD**-0.5 * LOG2E
    strips = 4
    wide = q.shape[1] // strips
    some = wide // own

    def s_copy(h):
        here = pl.ds(h * group * HEAD, group * HEAD)
        return pltpu.make_async_remote_copy(seen.at[0, here], seen.at[1, here], s_send.at[h], s_recv.at[h], device_id=mate,
                                            device_id_type=MESH)

    def attend(h, blocks, first, final):
        ones = jnp.ones((8, 2 * own * len(blocks)), BF16)
        if first:
            ok = (lax.broadcasted_iota(jnp.int32, (own, wide), 1) & (own - 1)) >= lax.broadcasted_iota(jnp.int32, (own, wide), 0)

        def seen_by(s):
            t = s * 2 // strips
            return [(j, u) for n_j, j in enumerate(blocks) for u in range(2) if not first or n_j or u <= t], t

        def score(s):
            keys = jnp.concatenate([kv[j, h, u, 0] for j, u in seen_by(s)[0]], axis=0)
            return _dot(keys, q[h, pl.ds(s * wide, wide), :], 1, 1)

        scores, parts = {s: score(s) for s in range(2)}, {}

        def mix(s):
            at = pl.ds(s * wide, wide)
            p, keep = parts.pop(s)
            these, t = seen_by(s)
            values = jnp.concatenate([kv[j, h, u, 1] for j, u in these], axis=1)
            new = _dot(jnp.concatenate([values, ones[:, : values.shape[1]]], axis=0), p)
            if not first:
                new = mix_s[h, :, at] * keep + new
            if not final:
                mix_s[h, :, at] = new
                return
            o = (new[:HEAD] * (1 / new[HEAD : HEAD + 1])).astype(BF16)
            for i in range(some):
                row = pl.multiple_of((h * group + s % (strips // 2) * some + i) * HEAD, HEAD)
                seen[0, pl.ds(row, HEAD), t * own : (t + 1) * own] = o[:, i * own : (i + 1) * own]

        for s in range(strips):
            at = pl.ds(s * wide, wide)
            if s + 2 < strips:
                scores[s + 2] = score(s + 2)
            sc, keep, t = scores.pop(s), None, s * 2 // strips
            if first:
                here = jnp.where(ok, sc[t * own : (t + 1) * own], HIDDEN)
                sc = jnp.concatenate([x for x in (sc[: t * own], here, sc[(t + 1) * own :]) if x.shape[0]], axis=0)
            top = sc.max(axis=0, keepdims=True)
            if not first:
                old = top_s[h, :, at]
                top = jnp.maximum(old, top)
                keep = jnp.exp2((old - top) * e)
            if not final:
                top_s[h, :, at] = top
            parts[s] = jnp.exp2((sc - top) * e).astype(BF16), keep
            if s > 1:
                mix(s - 2)
        for s in range(strips - 2, strips):
            mix(s)
        if final:
            s_copy(h).start()

    def take(block, h, only=None):
        with scope("arrive"):
            for t in (t0, t1) if only is None else (only,):
                arrived(block, t, h)

    def near(h):
        take(prev, h, (t1, t0)[h])

        @pl.when(chip == last)
        def _():
            take(prev, h, (t0, t1)[h])

        with scope("att_2f"):
            if h == 0:
                turn_queries(nq - 1)
            attend(h, [chip, prev], True, False)

    def only(h, _):
        @pl.when(chip == 1)
        def _():
            @pl.when(h > 0)
            def _():
                take(prev, h)

            with scope("att_2ff"):
                attend(h, [chip, prev], True, True)

        @pl.when(chip == 0)
        def _():
            with scope("att_1f"):
                attend(h, [chip], True, True)

    def far(h, _):
        @pl.when(chip == last)
        def _():
            @pl.when(h == 0)
            def _():
                take(0, h)

            take(1, h)
            with scope("att_2"):
                attend(h, [0, 1], False, True)

        @pl.when(chip == 2)
        def _():
            take(0, h)
            with scope("att_1"):
                attend(h, [0], False, True)

    @pl.when(chip > 1)
    def _():
        for h in range(hk):
            near(h)
        lax.fori_loop(0, hk, far, None)

    @pl.when(chip < 2)
    def _():
        turn_queries(nq - 1)
        lax.fori_loop(0, hk, only, None)

    def weight(i, side):
        return wob[i, pl.ds(side, half), :]

    def y_give(i, side):
        return pltpu.make_async_remote_copy(ys.at[pl.ds(theirs, own), pl.ds(i * part, part)],
                                            out_ref.at[:, pl.ds(pl.multiple_of(side + i * part, part), part)],
                                            y_send.at[i], y_recv.at[i], device_id=mate, device_id_type=MESH)

    def partial(i, c, rows_at):
        side = (cols, mate_cols)[c]
        return _dot(seen[c, :, rows_at], weight(i, side), 0, 0)

    with scope("r_wait"):
        r_copy.wait()
        r_give.wait_recv()
        for i in range(nq):
            o_copy(i).wait()
    every, it, me_at = slice(None), pl.ds(theirs, own), pl.ds(mine, own)
    for i in range(nq - 1):
        at = slice(i * part, (i + 1) * part)
        with scope("o_first"):
            acc[:, at] = xr[:, at].astype(F32) + partial(i, 0, every)
    with scope("seen_wait"):
        for h in range(hk):
            s_copy(h).wait_recv()
    with scope("o_second"):
        for i in range(nq - 1):
            at = slice(i * part, (i + 1) * part)
            ys[:, at] = (acc[:, at] + partial(i, 1, every)).astype(BF16)
    for i in range(nq - 1):
        y_give(i, cols).start()
    at = pl.ds((nq - 1) * part, part)
    with scope("o_theirs"):
        ys[it, at] = (xr[it, at].astype(F32) + partial(nq - 1, 0, it) + partial(nq - 1, 1, it)).astype(BF16)
    y_give(nq - 1, cols).start()
    with scope("o_mine"):
        out_ref[:, pl.ds(cols, half - part)] = ys[me_at, : half - part]
        out_ref[:, pl.ds(pl.multiple_of(cols + (nq - 1) * part, part), part)] = (
            xr[me_at, at].astype(F32) + partial(nq - 1, 0, me_at) + partial(nq - 1, 1, me_at)).astype(BF16)

    with scope("y_wait"):
        for i in range(nq):
            y_give(i, cols).wait_send()
            y_give(i, mate_cols).wait_recv()
    for i in range(nx):
        a_copy(i, mine).wait_send()
    r_give.wait_send()
    for h in range(hk):
        s_copy(h).wait_send()

    def sent(flag, *copies):
        @pl.when(flag)
        def _():
            for copy in copies:
                copy.wait_send()

    both = [(w, h) for w in range(3) for h in range(hk)]
    sent(sends, *(to_next(w, h) for w, h in both))
    sent(wraps, *(to_last(w, h) for w, h in both))
    sent(backs, *(to_first(w) for w in range(3)))
    sent(relays, *(relay(t) for t in range(2)))
    sent(edges, *(edge(t) for t in range(2)))


def _call(x, gain, wq, wk, wv, wo, devices):
    own, d = x.shape
    n, toks = devices // 2, 2 * own
    half, kc = wq.shape[1] // 2, wk.shape[1] // 2
    nq, nx = 4, 2
    part = half // nq
    hk, group = kc // HEAD, half // kc
    cols = group * toks
    if (n, hk) != (4, 2):
        raise ValueError("group size")
    dma = pltpu.SemaphoreType.DMA
    any_ = pl.BlockSpec(memory_space=pltpu.HBM)
    return pl.pallas_call(
        functools.partial(_kernel, n),
        out_shape=pltpu.VMEM((own, d), BF16),
        in_specs=[any_] * 6,
        out_specs=pl.BlockSpec(memory_space=pltpu.VMEM),
        scratch_shapes=[
            pltpu.VMEM((d,), BF16),
            pltpu.VMEM((own, d), BF16),
            pltpu.VMEM((toks, d), BF16),
            pltpu.VMEM((toks, half), BF16),
            pltpu.VMEM((d, 2 * kc), BF16),
            pltpu.VMEM((nq, d, part), BF16),
            pltpu.VMEM((nq, d, part), BF16),
            pltpu.VMEM((nq, toks, part), BF16),
            pltpu.VMEM((hk, cols, HEAD), BF16),
            pltpu.VMEM((n, hk, 2, 2, HEAD, HEAD), BF16),
            pltpu.VMEM((2, half, toks), BF16),
            pltpu.VMEM((toks, half), F32),
            pltpu.VMEM((toks, half), BF16),
            pltpu.VMEM((hk, 1, cols), F32),
            pltpu.VMEM((hk, HEAD + 8, cols), F32),
            pltpu.VMEM((toks, HEAD), F32),
            pltpu.VMEM((toks, HEAD), F32),
            dma, dma((nx,)), dma((2,)), dma((nq,)), dma((nq,)),
            dma((nx,)), dma((nx,)), dma, dma, dma,
            dma((3, hk)), dma((3, hk)), dma((3,)), dma((2,)), dma((2,)), dma((n, 2, hk)),
            dma((hk,)), dma((hk,)),
            dma((nq,)), dma((nq,)),
        ],
        compiler_params=pltpu.CompilerParams(collective_id=0, has_side_effects=True, vmem_limit_bytes=VMEM),
    )(x, gain, wq, wk, wv, wo)


def solution(mesh):
    devices = mesh.shape["sp"]

    def step(x, gain, wq, wk, wv, wo):
        return _call(x, gain, wq, wk, wv, wo, devices)

    tokens, whole = P(("dp", "sp"), None), P(None, None)
    return jax.shard_map(
        step,
        mesh=mesh,
        in_specs=(tokens, P(None), whole, whole, whole, whole),
        out_specs=tokens,
        check_vma=False,
    )
```

```python
import functools

import jax
import jax.numpy as jnp
from jax import lax
from jax.experimental import pallas as pl
from jax.experimental.pallas import tpu as pltpu
from jax.sharding import PartitionSpec as P

HEAD = 128
THETA = 10000
LOG2E = 1.4426950408889634
LOG2T = 13.287712379549449
HIDDEN = -2e30
VMEM = 60 * 2**20
MESH = pl.DeviceIdType.MESH
F32, BF16 = jnp.float32, jnp.bfloat16
scope = jax.named_scope


def _dot(a, b, ca=1, cb=0):
    return lax.dot_general(a, b, (((ca,), (cb,)), ((), ())), preferred_element_type=F32)


def _kernel(n, x_hbm, gain_hbm, wq_hbm, wk_hbm, wv_hbm, wo_hbm, out_ref,
            gain_s, xb, a, xr, wkv, wqb, wob, raw, q, kv, seen, acc, ys, top_s, mix_s, cos_s, sin_s,
            g_sem, x_sem, wkv_sem, wq_sem, wo_sem, a_send, a_recv, r_sem, r_send, r_recv,
            k_next, k_wrap, k_back, k_relay, k_edge, k_recv, s_send, s_recv, y_send, y_recv):
    own, d = x_hbm.shape
    toks = 2 * own
    nq, _, part = wqb.shape
    half = nq * part
    hk = kv.shape[1]
    kc = hk * HEAD
    group = q.shape[1] // toks
    me = lax.axis_index("sp")
    chip, core = lax.div(me, 2), lax.rem(me, 2)
    mate = {"sp": chip * 2 + 1 - core}

    def peer(at):
        return {"sp": at * 2 + core}

    mine = pl.multiple_of(core * own, own)
    theirs = pl.multiple_of((1 - core) * own, own)
    cols = pl.multiple_of(core * half, half)
    mate_cols = pl.multiple_of((1 - core) * half, half)

    nx = x_sem.shape[0]
    rows = own // nx
    kcols = pl.ds(pl.multiple_of(core * kc, kc), kc)

    def x_copy(i):
        return pltpu.make_async_copy(x_hbm.at[pl.ds(i * rows, rows)], xb.at[pl.ds(i * rows, rows)], x_sem.at[i])

    def q_copy(i):
        return pltpu.make_async_copy(wq_hbm.at[:, pl.ds(pl.multiple_of(cols + i * part, part), part)], wqb.at[i], wq_sem.at[i])

    def o_copy(i):
        return pltpu.make_async_copy(wo_hbm.at[:, pl.ds(pl.multiple_of(cols + i * part, part), part)], wob.at[i], wo_sem.at[i])

    for i in range(nx):
        x_copy(i).start()
    g_copy = pltpu.make_async_copy(gain_hbm, gain_s, g_sem)
    g_copy.start()
    barrier = pltpu.get_barrier_semaphore()
    pl.semaphore_signal(barrier, inc=1, device_id=mate, device_id_type=MESH)
    for i in range(1, n):
        pl.semaphore_signal(barrier, inc=1, device_id=peer(lax.rem(chip + i, n)), device_id_type=MESH)

    k_copy = pltpu.make_async_copy(wk_hbm.at[:, kcols], wkv.at[:, pl.ds(0, kc)], wkv_sem.at[0])
    v_copy = pltpu.make_async_copy(wv_hbm.at[:, kcols], wkv.at[:, pl.ds(kc, kc)], wkv_sem.at[1])
    r_copy = pltpu.make_async_copy(x_hbm.at[:, pl.ds(cols, half)], xr.at[pl.ds(mine, own)], r_sem)
    r_give = pltpu.make_async_remote_copy(x_hbm.at[:, pl.ds(mate_cols, half)], xr.at[pl.ds(mine, own)], r_send, r_recv, device_id=mate,
                                          device_id_type=MESH)
    k_copy.start()

    lane = lax.broadcasted_iota(jnp.int32, (toks, HEAD), 1)
    place = lax.broadcasted_iota(jnp.int32, (toks, HEAD), 0) + chip * toks
    turn = lax.rem(lane, HEAD // 2).astype(F32) * (-LOG2T / (HEAD // 2))
    angle = place.astype(F32) * jnp.exp2(turn)
    cos_s[...] = jnp.cos(angle)
    sin_s[...] = jnp.where(lane < HEAD // 2, -1.0, 1.0) * jnp.sin(angle)
    v_copy.start()

    def turned(t, cos, sin):
        t = t.astype(BF16).astype(F32)
        return (t * cos + pltpu.roll(t, HEAD // 2, 1) * sin).astype(BF16)

    def early(i):
        @pl.when(chip == 0)
        def _():
            for j in range(i + 1, nq):
                q_copy(j).start(priority=1)

    def in_turn(i):
        @pl.when(chip > 0)
        def _():
            q_copy(i).start(priority=1)

    def a_copy(i, at):
        here = pl.ds(pl.multiple_of(at + i * rows, rows), rows)
        return pltpu.make_async_remote_copy(a.at[here], a.at[here], a_send.at[i], a_recv.at[i], device_id=mate, device_id_type=MESH)

    for i in range(nx):
        with scope("x_wait"):
            x_copy(i).wait()
        if i == 0:
            q_copy(0).start(priority=1)
            early(0)
            with scope("g_wait"):
                g_copy.wait()
            gain = gain_s[...].astype(F32)[None]
        wide = xb[pl.ds(i * rows, rows), :].astype(F32)
        scale = lax.rsqrt(jnp.mean(wide * wide, -1, keepdims=True) + 1e-6)
        a[pl.ds(pl.multiple_of(mine + i * rows, rows), rows), :] = (wide * scale * gain).astype(BF16)
        if i == 0:
            with scope("barrier"):
                pl.semaphore_wait(barrier, n)
        a_copy(i, mine).start()

    def piece(sem, block, t, h, to, half=None):
        ref = kv.at[block, h, t] if half is None else kv.at[block, h, t, half]
        return pltpu.make_async_remote_copy(ref, ref, sem, k_recv.at[block, t, h], device_id=peer(to), device_id_type=MESH)

    t0, t1 = core, 1 - core
    last = n - 1
    sends, wraps, backs = chip < last, chip == 0, chip == 1
    relays, edges = (chip > 0) & (chip < last), (chip == 0) | (chip == last)
    edge_block, edge_to = jnp.where(chip == 0, 1, 0), jnp.where(chip == 0, last, last - 1)
    prev, nxt = lax.rem(chip + n - 1, n), lax.rem(chip + 1, n)

    def to_next(w, h):
        return piece(k_next.at[w, h], chip, t1 if w == 2 else t0, h, nxt, None if w == 2 else w)

    def to_last(w, h):
        return piece(k_wrap.at[w, h], chip, t1 if w == 2 else t0, h, last, None if w == 2 else w)

    def to_first(w):
        return piece(k_back.at[w], chip, t1 if w == 2 else t0, 0 if w == 2 else 1, 0, None if w == 2 else w)

    def relay_head(i):
        return jnp.where(chip == 1, 0, i)

    def relay(i):
        return piece(k_relay.at[i], prev, (t0, t1)[i], relay_head(i), nxt)

    def edge_head(i):
        return jnp.where(chip == 0, 1 - i, 1)

    def edge(i):
        return piece(k_edge.at[i], edge_block, (t0, t1)[i], edge_head(i), edge_to)

    def arrived(block, t, h):
        piece(k_edge.at[0], block, t, h, chip).wait_recv()

    def when(flag, *copies):
        @pl.when(flag)
        def _():
            for copy in copies:
                copy.start()

    def keys(r, t):
        here = pl.ds(pl.multiple_of(t * own, own), own)
        cos, sin = cos_s[here, :], sin_s[here, :]
        for h in range(hk):
            kv[chip, h, t, 0] = turned(r[:, h * HEAD : (h + 1) * HEAD], cos, sin)

    def values(r, t):
        for h in range(hk):
            kv[chip, h, t, 1] = r[:, h * HEAD : (h + 1) * HEAD].astype(BF16).T

    def send(w):
        when(sends, *(to_next(w, h) for h in range(hk)))
        when(wraps, *(to_last(w, h) for h in reversed(range(hk))))
        when(backs, to_first(w))

    def own_product(columns):
        rows_at, mid = pl.ds(mine, own), d // 2
        return _dot(a[rows_at, :mid], wkv[:mid, columns]) + _dot(a[rows_at, mid:], wkv[mid:, columns])

    with scope("k_wait"):
        k_copy.wait()
    with scope("k_mm"):
        keys(own_product(slice(0, kc)), t0)
    send(0)
    with scope("v_wait"):
        v_copy.wait()
    in_turn(1)
    with scope("v_mm"):
        values(own_product(slice(kc, 2 * kc)), t0)
    send(1)

    def first_queries(at):
        here = pl.ds(at, own)
        raw[0, here, :] = _dot(a[here, :], wqb[0]).astype(BF16)

    def others():
        with scope("a_wait"):
            for j in range(nx):
                a_copy(j, theirs).wait_recv()
        with scope("kv_mm"):
            r = _dot(a[pl.ds(theirs, own), :], wkv[...])
            keys(r[:, :kc], t1)
            values(r[:, kc:], t1)
        send(2)

    def first_weights():
        with scope("q_wait"):
            q_copy(0).wait()
        in_turn(2)

    def second_weights():
        in_turn(3)
        with scope("q_wait"):
            q_copy(1).wait()
        o_copy(0).start(priority=1)

    heads = part // HEAD

    def turn_queries(i):
        for j in range(heads):
            at = i * heads + j
            for t in range(2):
                here = slice(t * own, (t + 1) * own)
                q[at // group, pl.ds((t * group + at % group) * own, own), :] = turned(
                    raw[i, here, j * HEAD : (j + 1) * HEAD], cos_s[here, :], sin_s[here, :])

    def relay_step(i, flag):
        @pl.when(flag)
        def _():
            with scope("relay_wait"):
                arrived(prev, (t0, t1)[i], relay_head(i))
            relay(i).start()

    def edge_step(i, flag):
        @pl.when(flag)
        def _():
            with scope("edge_wait"):
                arrived(edge_block, (t0, t1)[i], edge_head(i))
            edge(i).start()

    e = HEAD**-0.5 * LOG2E
    strips = 4
    wide = q.shape[1] // strips
    some = wide // own

    def s_copy(h):
        here = pl.ds(h * group * HEAD, group * HEAD)
        return pltpu.make_async_remote_copy(seen.at[0, here], seen.at[1, here], s_send.at[h], s_recv.at[h], device_id=mate,
                                            device_id_type=MESH)

    def attend(h, blocks, first, final):
        ones = jnp.ones((8, 2 * own * len(blocks)), BF16)
        if first:
            ok = (lax.broadcasted_iota(jnp.int32, (own, wide), 1) & (own - 1)) >= lax.broadcasted_iota(jnp.int32, (own, wide), 0)

        def seen_by(s):
            t = s * 2 // strips
            return [(j, u) for n_j, j in enumerate(blocks) for u in range(2) if not first or n_j or u <= t], t

        def score(s):
            keys = jnp.concatenate([kv[j, h, u, 0] for j, u in seen_by(s)[0]], axis=0)
            return _dot(keys, q[h, pl.ds(s * wide, wide), :], 1, 1)

        scores, parts = {s: score(s) for s in range(2)}, {}

        def mix(s):
            at = pl.ds(s * wide, wide)
            p, keep = parts.pop(s)
            these, t = seen_by(s)
            values = jnp.concatenate([kv[j, h, u, 1] for j, u in these], axis=1)
            new = _dot(jnp.concatenate([values, ones[:, : values.shape[1]]], axis=0), p)
            if not first:
                new = mix_s[h, :, at] * keep + new
            if not final:
                mix_s[h, :, at] = new
                return
            o = (new[:HEAD] * (1 / new[HEAD : HEAD + 1])).astype(BF16)
            for i in range(some):
                row = pl.multiple_of((h * group + s % (strips // 2) * some + i) * HEAD, HEAD)
                seen[0, pl.ds(row, HEAD), t * own : (t + 1) * own] = o[:, i * own : (i + 1) * own]

        for s in range(strips):
            at = pl.ds(s * wide, wide)
            if s + 2 < strips:
                scores[s + 2] = score(s + 2)
            sc, keep, t = scores.pop(s), None, s * 2 // strips
            if first:
                here = jnp.where(ok, sc[t * own : (t + 1) * own], HIDDEN)
                sc = jnp.concatenate([x for x in (sc[: t * own], here, sc[(t + 1) * own :]) if x.shape[0]], axis=0)
            top = sc.max(axis=0, keepdims=True)
            if not first:
                old = top_s[h, :, at]
                top = jnp.maximum(old, top)
                keep = jnp.exp2((old - top) * e)
            if not final:
                top_s[h, :, at] = top
            parts[s] = jnp.exp2((sc - top) * e).astype(BF16), keep
            if s > 1:
                mix(s - 2)
        for s in range(strips - 2, strips):
            mix(s)
        if final:
            s_copy(h).start()

    @pl.when(core == 0)
    def _():
        others()
        first_weights()
        with scope("q_mm"):
            raw[0] = _dot(a[...], wqb[0]).astype(BF16)
        second_weights()
        with scope("q_mm"):
            raw[1] = _dot(a[...], wqb[1]).astype(BF16)
            turn_queries(0)

    @pl.when(core == 1)
    def _():
        first_weights()
        with scope("q_own"):
            first_queries(mine)
        others()
        second_weights()
        with scope("q_mm"):
            first_queries(theirs)
            raw[1] = _dot(a[...], wqb[1]).astype(BF16)
            turn_queries(0)

    r_copy.start(priority=1)
    r_give.start()
    for i in range(1, nq):
        if i > 1:
            with scope("q_wait"):
                q_copy(i).wait()
            if i + 1 < nq:
                o_copy(i + 1).start(priority=1)
            with scope("q_mm"):
                raw[i] = _dot(a[...], wqb[i]).astype(BF16)
                turn_queries(i - 1)
        else:
            o_copy(1).start(priority=1)
            o_copy(2).start(priority=1)
        if i == 1:
            relay_step(0, relays)

            @pl.when(chip == 0)
            def _():
                turn_queries(1)
                with scope("att_1f"):
                    attend(0, [chip], True, True)

            edge_step(1, wraps)
        if i == 2:
            relay_step(1, chip == 1)
            edge_step(0, edges)
        if i == 3:
            relay_step(1, chip == 2)
            edge_step(1, chip == last)

    def take(block, h, only=None):
        with scope("arrive"):
            for t in (t0, t1) if only is None else (only,):
                arrived(block, t, h)

    def near(h):
        take(prev, h, (t1, t0)[h])

        @pl.when(chip == last)
        def _():
            take(prev, h, (t0, t1)[h])

        with scope("att_2f"):
            if h == 0:
                turn_queries(nq - 1)
            attend(h, [chip, prev], True, False)

    def only(h, _):
        @pl.when(chip == 1)
        def _():
            @pl.when(h > 0)
            def _():
                take(prev, h)

            with scope("att_2ff"):
                attend(h, [chip, prev], True, True)

        @pl.when((chip == 0) & (h > 0))
        def _():
            with scope("att_1f"):
                attend(h, [chip], True, True)

    def far(h, _):
        @pl.when(chip == last)
        def _():
            @pl.when(h == 0)
            def _():
                take(0, h)

            take(1, h)
            with scope("att_2"):
                attend(h, [0, 1], False, True)

        @pl.when(chip == 2)
        def _():
            take(0, h)
            with scope("att_1"):
                attend(h, [0], False, True)

    @pl.when(chip > 1)
    def _():
        for h in range(hk):
            near(h)
        lax.fori_loop(0, hk, far, None)

    @pl.when(chip < 2)
    def _():
        turn_queries(nq - 1)
        lax.fori_loop(0, hk, only, None)

    def weight(i, side):
        return wob[i, pl.ds(side, half), :]

    def y_give(i, side):
        return pltpu.make_async_remote_copy(ys.at[pl.ds(theirs, own), pl.ds(i * part, part)],
                                            out_ref.at[:, pl.ds(pl.multiple_of(side + i * part, part), part)],
                                            y_send.at[i], y_recv.at[i], device_id=mate, device_id_type=MESH)

    def partial(i, c, rows_at):
        side = (cols, mate_cols)[c]
        return _dot(seen[c, :, rows_at], weight(i, side), 0, 0)

    with scope("r_wait"):
        r_copy.wait()
        r_give.wait_recv()
        for i in range(nq):
            o_copy(i).wait()
    every, it, me_at = slice(None), pl.ds(theirs, own), pl.ds(mine, own)
    for i in range(nq - 1):
        at = slice(i * part, (i + 1) * part)
        with scope("o_first"):
            acc[:, at] = xr[:, at].astype(F32) + partial(i, 0, every)
    with scope("seen_wait"):
        for h in range(hk):
            s_copy(h).wait_recv()
    with scope("o_second"):
        for i in range(nq - 1):
            at = slice(i * part, (i + 1) * part)
            ys[:, at] = (acc[:, at] + partial(i, 1, every)).astype(BF16)
    for i in range(nq - 1):
        y_give(i, cols).start()
    at = pl.ds((nq - 1) * part, part)
    with scope("o_theirs"):
        ys[it, at] = (xr[it, at].astype(F32) + partial(nq - 1, 0, it) + partial(nq - 1, 1, it)).astype(BF16)
    y_give(nq - 1, cols).start()
    with scope("o_mine"):
        out_ref[:, pl.ds(cols, half - part)] = ys[me_at, : half - part]
        out_ref[:, pl.ds(pl.multiple_of(cols + (nq - 1) * part, part), part)] = (
            xr[me_at, at].astype(F32) + partial(nq - 1, 0, me_at) + partial(nq - 1, 1, me_at)).astype(BF16)

    with scope("y_wait"):
        for i in range(nq):
            y_give(i, cols).wait_send()
            y_give(i, mate_cols).wait_recv()
    for i in range(nx):
        a_copy(i, mine).wait_send()
    r_give.wait_send()
    for h in range(hk):
        s_copy(h).wait_send()

    def sent(flag, *copies):
        @pl.when(flag)
        def _():
            for copy in copies:
                copy.wait_send()

    both = [(w, h) for w in range(3) for h in range(hk)]
    sent(sends, *(to_next(w, h) for w, h in both))
    sent(wraps, *(to_last(w, h) for w, h in both))
    sent(backs, *(to_first(w) for w in range(3)))
    sent(relays, *(relay(t) for t in range(2)))
    sent(edges, *(edge(t) for t in range(2)))


def _call(x, gain, wq, wk, wv, wo, devices):
    own, d = x.shape
    n, toks = devices // 2, 2 * own
    half, kc = wq.shape[1] // 2, wk.shape[1] // 2
    nq, nx = 4, 2
    part = half // nq
    hk, group = kc // HEAD, half // kc
    cols = group * toks
    if (n, hk) != (4, 2):
        raise ValueError("group size")
    dma = pltpu.SemaphoreType.DMA
    any_ = pl.BlockSpec(memory_space=pltpu.HBM)
    return pl.pallas_call(
        functools.partial(_kernel, n),
        out_shape=pltpu.VMEM((own, d), BF16),
        in_specs=[any_] * 6,
        out_specs=pl.BlockSpec(memory_space=pltpu.VMEM),
        scratch_shapes=[
            pltpu.VMEM((d,), BF16),
            pltpu.VMEM((own, d), BF16),
            pltpu.VMEM((toks, d), BF16),
            pltpu.VMEM((toks, half), BF16),
            pltpu.VMEM((d, 2 * kc), BF16),
            pltpu.VMEM((nq, d, part), BF16),
            pltpu.VMEM((nq, d, part), BF16),
            pltpu.VMEM((nq, toks, part), BF16),
            pltpu.VMEM((hk, cols, HEAD), BF16),
            pltpu.VMEM((n, hk, 2, 2, HEAD, HEAD), BF16),
            pltpu.VMEM((2, half, toks), BF16),
            pltpu.VMEM((toks, half), F32),
            pltpu.VMEM((toks, half), BF16),
            pltpu.VMEM((hk, 1, cols), F32),
            pltpu.VMEM((hk, HEAD + 8, cols), F32),
            pltpu.VMEM((toks, HEAD), F32),
            pltpu.VMEM((toks, HEAD), F32),
            dma, dma((nx,)), dma((2,)), dma((nq,)), dma((nq,)),
            dma((nx,)), dma((nx,)), dma, dma, dma,
            dma((3, hk)), dma((3, hk)), dma((3,)), dma((2,)), dma((2,)), dma((n, 2, hk)),
            dma((hk,)), dma((hk,)),
            dma((nq,)), dma((nq,)),
        ],
        compiler_params=pltpu.CompilerParams(collective_id=0, has_side_effects=True, vmem_limit_bytes=VMEM),
    )(x, gain, wq, wk, wv, wo)


def solution(mesh):
    devices = mesh.shape["sp"]

    def step(x, gain, wq, wk, wv, wo):
        return _call(x, gain, wq, wk, wv, wo, devices)

    tokens, whole = P(("dp", "sp"), None), P(None, None)
    return jax.shard_map(
        step,
        mesh=mesh,
        in_specs=(tokens, P(None), whole, whole, whole, whole),
        out_specs=tokens,
        check_vma=False,
    )
```
